256 devices in a mesh: dp: 64 (over z, y, core), mp: 4 (over x).
Axes of the slice: x: 4, y: 4, z: 8, core: 2. Of those that a mesh axis runs over, the one named last changes fastest.
Arguments:
- pixels: bfloat16 [1024, 256, 768], P('dp', 'mp'), may hold values from -6 to 6
- selection: int32 [1024], P('dp'), may hold values from 0 to 1, as said below
- destination: int32 [1024], P('dp'), may hold values from 0 to 63, as said below
- patch_weight: bfloat16 [768, 1024], replicated, may hold values from -0.21875 to 0.21875
- position: bfloat16 [256, 1024], P('mp'), may hold values from -6 to 6
- query_key_value: bfloat16 [3, 1024, 1024], P(None, None, 'mp'), may hold values from -1 to 1
- output_weight: bfloat16 [1024, 1024], P('mp'), may hold values from -0.1875 to 0.1875
- up_weight: bfloat16 [1024, 4096], P(None, 'mp'), may hold values from -0.1875 to 0.1875
- down_weight: bfloat16 [4096, 1024], P('mp'), may hold values from -0.09375 to 0.09375
- norm_gains: float32 [3, 1024], replicated, may hold values from 0.25 to 1.75
- embedding_weight: bfloat16 [1024, 1024], replicated, may hold values from -0.1875 to 0.1875
- caption_vectors: bfloat16 [1024, 1024], P('dp'), may hold values from -6 to 6
- loss_params: float32 [2], replicated, may hold values from -1 to 1
Outputs:
- image_embedding: float32 [256, 1024], P('dp')
- pair_loss: float32 [256], P('dp')
The draws below stay inside these ranges and needn't reach their ends.
Inputs may be any that keep to these rules, and one draw needn't show every extreme that they name: `selection`: exactly 128 examples are selected in all; each index of dp holds between 1 and 3 of them, and some holds exactly 3. Among selected examples, at most 4 have the same destination, some destination has exactly 4, and no index of dp holds two selected examples with the same destination. Destinations of unselected examples are arbitrary.
All inputs are finite; a program needn't handle non-finite values.
Results may differ from the reference program's by a relative error of at most 0.0031.
Values may be sent and summed in bfloat16 or wider, within the bound.
A program may use at most 128 MiB of HBM per device.

```python
import jax
import jax.numpy as jnp
from jax import lax

D = 1024
HEADS = 16
HEAD_DIM = 64
FF = 4096
PATCHES = 256
EMBED = 1024
PATCH = 768
EX_DEV = 16
SEL_DEV = 2
SEND_MOST = 3
RECV_MOST = 4
EXAMPLES = 1024
SELECTED = 128
LEARN_SLOTS = 256
N_DP = 64


def routing_plan(key):
    folded = jax.random.fold_in(key, 11)
    subkeys = jax.random.split(folded, 6)
    halfway = N_DP // 2
    leading = jax.random.randint(subkeys[0], (halfway,), 1, SEND_MOST + 1).at[0].set(SEND_MOST)
    counts = jnp.concatenate([leading, 2 * SEL_DEV - leading])[jax.random.permutation(subkeys[1], N_DP)]
    orders = jax.vmap(lambda subkey: jax.random.permutation(subkey, EX_DEV))(jax.random.split(subkeys[2], N_DP))
    chosen = (orders < counts[:, None]).reshape(EXAMPLES).astype(jnp.int32)
    ranking = jnp.cumsum(chosen) - 1
    load_first = jax.random.randint(subkeys[3], (halfway,), 0, RECV_MOST + 1).at[0].set(RECV_MOST)
    receiver_loads = jnp.concatenate([load_first, 2 * SEL_DEV - load_first])[jax.random.permutation(subkeys[4], N_DP)]
    boundaries = jnp.cumsum(receiver_loads)
    stride = SELECTED // RECV_MOST
    places = ranking % stride * RECV_MOST + ranking // stride
    listed = jnp.sum((boundaries[None, :] <= places[:, None]).astype(jnp.int32), axis=1)
    filler = jax.random.randint(subkeys[5], (EXAMPLES,), 0, N_DP)
    targets = jnp.where(chosen > 0, listed, filler).astype(jnp.int32)
    return (chosen, targets)


def draw_selection(key, part):
    return routing_plan(key)[0]


def draw_destination(key, part):
    return routing_plan(key)[1]


def draw_query_key_value(key, part):
    folded = jax.random.fold_in(key, 23)
    subkeys = jax.random.split(folded, 1)
    values = jax.random.normal(subkeys[0], (3, D, D), jnp.float32) * D ** (-0.5)
    return jnp.clip(values, -1.0, 1.0).astype(jnp.bfloat16)


def steps_of(key, extent, cuts, least, high):
    loudness, own = 1.0, jax.random.fold_in(key, 6)
    for dim, shards_of in cuts:
        heights = jnp.exp(jax.random.uniform(jax.random.fold_in(own, dim), (shards_of,), jnp.float32, least / len(cuts), high / len(cuts)))
        loudness = loudness * jnp.repeat(heights, extent[dim] // shards_of).reshape([-1 if axis == dim else 1 for axis in range(len(extent))])
    return loudness


def normal_values(stream_key, dims, scale, limit, cuts=(), kind=jnp.bfloat16):
    array = scale * jax.random.normal(stream_key, dims, jnp.float32)
    if cuts:
        array = array * steps_of(stream_key, dims, cuts, -0.22, 0.18)
    return jnp.clip(array, -limit, limit).astype(kind)


def setup_inputs(seed: int = 0) -> dict:
    key_list = jax.random.split(jax.random.key(seed), 14)
    return {
        "pixels": normal_values(key_list[0], (EXAMPLES, PATCHES, PATCH), 1.0, 6.0, ((0, 64), (1, 4))),
        "selection": draw_selection(jax.random.fold_in(key_list[13], 71), 0),
        "destination": draw_destination(jax.random.fold_in(key_list[13], 71), 0),
        "patch_weight": normal_values(key_list[3], (PATCH, D), PATCH ** -0.5, 0.21875),
        "position": normal_values(key_list[4], (PATCHES, D), 1.0, 6.0, ((0, 4),)),
        "query_key_value": draw_query_key_value(jax.random.fold_in(key_list[13], 71), 0),
        "output_weight": normal_values(key_list[6], (D, D), D ** -0.5, 0.1875, ((0, 4),)),
        "up_weight": normal_values(key_list[7], (D, FF), D ** -0.5, 0.1875, ((1, 4),)),
        "down_weight": normal_values(key_list[8], (FF, D), FF ** -0.5, 0.09375, ((0, 4),)),
        "norm_gains": jnp.clip(1.0 + 0.15 * jax.random.normal(key_list[9], (3, D), jnp.float32), 0.25, 1.75),
        "embedding_weight": normal_values(key_list[10], (D, EMBED), D ** -0.5, 0.1875),
        "caption_vectors": normal_values(key_list[11], (EXAMPLES, EMBED), 1.0, 6.0, ((0, 64),)),
        "loss_params": jnp.clip(jax.random.uniform(key_list[12], (2,), jnp.float32, -1.0, 1.0), -1.0, 1.0),
    }


EPS = 1e-06

def layer_norm(values, gain):
    center = lax.optimization_barrier(jnp.mean(values, axis=-1, keepdims=True))
    centred = values - center
    spread = lax.optimization_barrier(jnp.mean(centred * centred, axis=-1, keepdims=True))
    return centred * lax.rsqrt(spread + EPS) * gain.astype(jnp.float32)

def unit_rows(values):
    scale = lax.rsqrt(lax.optimization_barrier(jnp.mean(values * values, axis=-1, keepdims=True)) + EPS)
    return values * scale * values.shape[-1] ** (-0.5)

def encode_image(image, patch_weight, position, qkv_flat, output_weight, up_weight, down_weight, norm_gains):
    hidden = jnp.dot(image, patch_weight, preferred_element_type=jnp.float32) + position.astype(jnp.float32)
    normed = layer_norm(hidden, norm_gains[0]).astype(jnp.bfloat16)
    projected = jnp.dot(normed, qkv_flat, preferred_element_type=jnp.float32).astype(jnp.bfloat16)
    shaped = projected.reshape(PATCHES, 3, HEADS, HEAD_DIM).astype(jnp.float32)
    query_rows = shaped[:, 0]
    key_rows = shaped[:, 1]
    value_rows = shaped[:, 2]
    scores = jnp.einsum('qhd,khd->hqk', query_rows, key_rows) * HEAD_DIM ** (-0.5)
    weights = jax.nn.softmax(scores, axis=-1).astype(jnp.bfloat16)
    context = jnp.einsum('hqk,khd->qhd', weights.astype(jnp.float32), value_rows).astype(jnp.bfloat16)
    context = context.reshape(PATCHES, D)
    hidden = hidden + jnp.dot(context, output_weight, preferred_element_type=jnp.float32)
    normed = layer_norm(hidden, norm_gains[1]).astype(jnp.bfloat16)
    expanded = jax.nn.gelu(jnp.dot(normed, up_weight, preferred_element_type=jnp.float32)).astype(jnp.bfloat16)
    hidden = hidden + jnp.dot(expanded, down_weight, preferred_element_type=jnp.float32)
    return lax.optimization_barrier(jnp.mean(hidden, axis=0))

def pair_terms(embedded, slot_example, texts, text_ids, text_live, loss_params, live, total):
    images = unit_rows(embedded)
    captions = unit_rows(texts)
    scale = 10.0 * jnp.exp(loss_params[0])
    shift = 2.0 * loss_params[1]
    logits = scale * jnp.dot(images, captions.T, precision=lax.Precision.HIGHEST) + shift
    signs = jnp.where(slot_example[:, None] == text_ids[None, :], 1.0, -1.0).astype(jnp.float32)
    terms = jax.nn.softplus(-signs * logits) * text_live[None, :].astype(jnp.float32)
    return jnp.where(live, lax.optimization_barrier(jnp.sum(terms, axis=1)) / total, 0.0).astype(jnp.float32)

def reference(pixels, selection, destination, patch_weight, position, query_key_value, output_weight, up_weight, down_weight, norm_gains, embedding_weight, caption_vectors, loss_params):
    indices = jnp.arange(EXAMPLES, dtype=jnp.int32)
    chosen = selection > 0
    ranking = (jnp.cumsum(selection) - 1).astype(jnp.int32)
    ordered = jnp.zeros((SELECTED,), jnp.int32).at[jnp.where(chosen, ranking, SELECTED).astype(jnp.int32)].set(indices, mode='drop')
    qkv_flat = query_key_value.transpose(1, 0, 2).reshape(D, 3 * D)

    def encode_one(example):
        return encode_image(pixels[example], patch_weight, position, qkv_flat, output_weight, up_weight, down_weight, norm_gains)
    pooled_list = lax.map(encode_one, ordered)
    hot = ((destination[:, None] == jnp.arange(N_DP, dtype=jnp.int32)[None, :]) & chosen[:, None]).astype(jnp.int32)
    running = jnp.cumsum(hot, axis=0)
    within = (lax.optimization_barrier(jnp.sum(running * hot, axis=1)) - 1).astype(jnp.int32)
    flat_slot = jnp.where(chosen, destination * RECV_MOST + within, LEARN_SLOTS).astype(jnp.int32)
    slot_rank = jnp.full((LEARN_SLOTS,), -1, jnp.int32).at[flat_slot].set(ranking, mode='drop')
    live = slot_rank >= 0
    safe_rank = jnp.maximum(slot_rank, 0).astype(jnp.int32)
    pooled = pooled_list[safe_rank]
    slot_example = jnp.where(live, ordered[safe_rank], -1).astype(jnp.int32)
    normed = layer_norm(pooled, norm_gains[2]).astype(jnp.bfloat16)
    embedded = jnp.dot(normed, embedding_weight, preferred_element_type=jnp.float32)
    embedded = jnp.where(live[:, None], embedded, 0.0).astype(jnp.float32)
    texts = caption_vectors[ordered].astype(jnp.float32)
    text_live = jnp.ones((SELECTED,), dtype=bool)
    losses = pair_terms(embedded, slot_example, texts, ordered, text_live, loss_params, live, float(SELECTED))
    return (embedded, losses)
```

```python
import jax
import jax.numpy as jnp
from jax import lax
from jax.sharding import PartitionSpec as P

HEAD_DIM = 64
PATCHES = 256
SEL_DEV = 2
SEND_MOST = 3
RECV_MOST = 4
EPS = 1e-06


def layer_norm(values, gain):
    center = jnp.mean(values, axis=-1, keepdims=True)
    centred = values - center
    spread = jnp.mean(centred * centred, axis=-1, keepdims=True)
    return centred * lax.rsqrt(spread + EPS) * gain


def unit_rows(values):
    scale = lax.rsqrt(jnp.mean(values * values, axis=-1, keepdims=True) + EPS)
    return values * scale * values.shape[-1] ** (-0.5)


def per_device(
    pixels, selection, destination, patch_weight, position, query_key_value, output_weight,
    up_weight, down_weight, norm_gains, embedding_weight, caption_vectors, loss_params,
):
    n_dp = lax.axis_size("dp")
    f32, bf16 = jnp.float32, jnp.bfloat16
    chosen = selection > 0
    local_rank = jnp.cumsum(selection) - 1
    picker = chosen[None, :] & (local_rank[None, :] == jnp.arange(SEND_MOST, dtype=jnp.int32)[:, None])
    live = jnp.any(picker, axis=1)
    dest = jnp.sum(jnp.where(picker, destination[None, :] + 1, 0), axis=1) - 1
    index = jnp.sum(jnp.where(picker, jnp.arange(selection.shape[0], dtype=jnp.int32)[None, :], 0), axis=1)

    captions = jnp.dot(picker.astype(bf16), caption_vectors, preferred_element_type=f32).astype(bf16)
    all_captions = lax.all_gather(captions, "dp", axis=0, tiled=True)
    all_dest = lax.all_gather(dest, "dp", axis=0, tiled=True)

    image = jnp.stack([lax.dynamic_index_in_dim(pixels, index[k], 0, keepdims=False) for k in range(SEND_MOST)])
    image = lax.all_gather(image, "mp", axis=1, tiled=True)
    place = lax.all_gather(position, "mp", axis=0, tiled=True)
    output_all = lax.all_gather(output_weight, "mp", axis=0, tiled=True)

    hidden = jnp.einsum("rpc,cd->rpd", image, patch_weight, preferred_element_type=f32) + place.astype(f32)[None]
    normed = layer_norm(hidden, norm_gains[0]).astype(bf16)
    projected = jnp.einsum("rpd,tdk->trpk", normed, query_key_value, preferred_element_type=f32).astype(bf16)
    heads = projected.shape[-1] // HEAD_DIM
    shaped = projected.reshape(3, SEND_MOST, PATCHES, heads, HEAD_DIM)
    scores = jnp.einsum("rqhd,rkhd->rhqk", shaped[0], shaped[1], preferred_element_type=f32) * HEAD_DIM ** (-0.5)
    weights = jax.nn.softmax(scores, axis=-1).astype(bf16)
    context = jnp.einsum("rhqk,rkhd->rqhd", weights, shaped[2], preferred_element_type=f32).astype(bf16)
    context = context.reshape(SEND_MOST, PATCHES, heads * HEAD_DIM)
    context = lax.all_gather(context, "mp", axis=0)
    segments = output_all.reshape(lax.axis_size("mp"), -1, output_all.shape[-1])
    hidden = hidden + jnp.einsum("mrpk,mkd->rpd", context, segments, preferred_element_type=f32)
    normed = layer_norm(hidden, norm_gains[1]).astype(bf16)
    expanded = jax.nn.gelu(jnp.einsum("rpd,df->rpf", normed, up_weight, preferred_element_type=f32)).astype(bf16)
    summed = jnp.sum(expanded.astype(f32), axis=1)
    part = jnp.dot(summed, down_weight.astype(f32), precision=lax.Precision.HIGHEST)
    rows = PATCHES // lax.axis_size("mp")
    own = lax.dynamic_slice_in_dim(hidden, lax.axis_index("mp") * rows, rows, axis=1)
    part = part + jnp.sum(own, axis=1)
    pooled = jnp.sum(lax.all_gather(part, "mp", axis=0), axis=0) / PATCHES
    normed = layer_norm(pooled, norm_gains[2]).astype(bf16)

    sorter = (dest[None, :] == jnp.arange(n_dp, dtype=jnp.int32)[:, None]) & live[None, :]
    outgoing = jnp.dot(sorter.astype(bf16), normed, preferred_element_type=f32).astype(bf16)
    arrived = lax.all_to_all(outgoing, "dp", split_axis=0, concat_axis=0, tiled=True)

    match = (all_dest == lax.axis_index("dp")).astype(jnp.int32).reshape(n_dp, SEND_MOST)
    present = jnp.sum(match, axis=1)
    place_of = jnp.cumsum(present) - present
    pick = (present[None, :] > 0) & (place_of[None, :] == jnp.arange(RECV_MOST, dtype=jnp.int32)[:, None])
    filled = jnp.any(pick, axis=1)
    slots = jnp.dot(pick.astype(bf16), arrived, preferred_element_type=f32).astype(bf16)
    embedded = jnp.dot(slots, embedding_weight, preferred_element_type=f32)
    embedded = jnp.where(filled[:, None], embedded, 0.0)
    scale = 10.0 * jnp.exp(loss_params[0])
    shift = 2.0 * loss_params[1]
    logits = scale * jnp.dot(
        unit_rows(embedded), unit_rows(all_captions.astype(f32)).T, precision=lax.Precision.HIGHEST
    ) + shift
    same = (pick[:, :, None] & (match[None] > 0)).reshape(RECV_MOST, n_dp * SEND_MOST)
    signs = jnp.where(same, 1.0, -1.0)
    terms = jax.nn.softplus(-signs * logits) * (all_dest >= 0).astype(f32)[None, :]
    losses = jnp.where(filled, jnp.sum(terms, axis=1) / float(n_dp * SEL_DEV), 0.0)
    return embedded, losses


def solution(mesh):
    in_specs = (
        P("dp", "mp", None), P("dp"), P("dp"), P(), P("mp", None), P(None, None, "mp"), P("mp", None),
        P(None, "mp"), P("mp", None), P(), P(), P("dp", None), P(),
    )
    out_specs = (P("dp", None), P("dp"))
    return jax.shard_map(per_device, mesh=mesh, in_specs=in_specs, out_specs=out_specs, check_vma=False)
```

```python
import functools

import jax
import jax.numpy as jnp
from jax import lax
from jax.experimental import pallas as pl
from jax.experimental.pallas import tpu as pltpu
from jax.sharding import PartitionSpec as P

EPS = 1e-06
SEND_MOST = 3
RECV_MOST = 4
SEL_DEV = 2
HEAD_DIM = 64
Y, CORES = 4, 2
F32, BF16 = jnp.float32, jnp.bfloat16
NT = (((1,), (1,)), ((), ()))


def norm_rows(values, gain):
    center = jnp.mean(values, axis=-1, keepdims=True)
    centred = values - center
    spread = jnp.mean(centred * centred, axis=-1, keepdims=True)
    return centred * lax.rsqrt(spread + EPS) * gain


def diagonal(rows):
    count = rows.shape[0]
    line = lax.broadcasted_iota(jnp.int32, (count, 128), 0) % 8
    out = jnp.zeros((count, 128), rows.dtype)
    for chunk in range(8):
        out = jnp.where(line == chunk, rows[:, chunk * 128 : (chunk + 1) * 128], out)
    return out


def dot(a, b):
    return jnp.dot(a, b, preferred_element_type=F32)


def body(
    n_dp, n_mp,
    selection, destination, loss_params, pixels, patch_weight, position, query_key_value, output_weight,
    up_weight, down_weight, gains, embedding_weight, captions,
    embedded_out, losses_out,
    pixels_v, patch_v, qkv_v, up_v, down_v, embedding_v, captions_v,
    pix, place, wo, hid, normed, qkv, ctx, cap_send, caps, caps_flat, summed, shared,
    out_send, arrived, picker, sign_of, weight_of,
    local, pix_s, pix_r, px_s, px_r, py_s, py_r, pc_s, pc_r, wx_s, wx_r, wy_s, wy_r, wc_s, wc_r,
    ctx_s, ctx_r, ar_s, ar_r, cap_s, cap_r, out_s, out_r,
):
    dp, mp = lax.axis_index("dp"), lax.axis_index("mp")
    right, left, opposite = (mp + 1) % n_mp, (mp + n_mp - 1) % n_mp, (mp + 2) % n_mp
    core, y, z = dp % CORES, (dp // CORES) % Y, dp // (CORES * Y)

    def on_y(step):
        return (z * Y + (y + step) % Y) * CORES + core

    partner = dp + 1 - 2 * core
    y_up, y_down, y_far = (y + 1) % Y, (y + Y - 1) % Y, (y + 2) % Y

    def remote(src, dst, sends, receives, where):
        return pltpu.make_async_remote_copy(
            src_ref=src, dst_ref=dst, send_sem=sends, recv_sem=receives, device_id=where,
            device_id_type=pl.DeviceIdType.MESH,
        )

    def arrival(ref, receives):
        remote(ref, ref, receives, receives, (dp, right)).wait_recv()

    pending = []

    def send(ref, sends, receives, where, src=None):
        src = ref if src is None else src
        remote(src, ref, sends, receives, where).start()
        pending.append((src, ref, sends, receives, where))

    loads = [
        (pixels, pixels_v), (captions, captions_v), (patch_weight, patch_v), (position, place.at[mp]),
        (query_key_value, qkv_v), (output_weight, wo.at[mp]), (up_weight, up_v), (down_weight, down_v),
        (embedding_weight, embedding_v),
    ]
    loads = [pltpu.make_async_copy(a, b, local.at[n]) for n, (a, b) in enumerate(loads)]
    for load in loads:
        load.start()

    barrier = pltpu.get_barrier_semaphore()

    def greet(step, carry):
        pl.semaphore_signal(barrier, inc=1, device_id=((dp + step) % n_dp, mp), device_id_type=pl.DeviceIdType.MESH)
        return carry

    for other in (right, left, opposite):
        pl.semaphore_signal(barrier, inc=1, device_id=(dp, other), device_id_type=pl.DeviceIdType.MESH)
    lax.fori_loop(1, n_dp, greet, 0)

    index = [jnp.int32(0)] * SEND_MOST
    target = [jnp.int32(-1)] * SEND_MOST
    count = jnp.int32(0)
    for example in range(selection.shape[0]):
        chosen = selection[example] > 0
        goal = destination[example]
        for k in range(SEND_MOST):
            hit = jnp.logical_and(chosen, count == k)
            index[k] = jnp.where(hit, example, index[k])
            target[k] = jnp.where(hit, goal, target[k])
        count = count + chosen.astype(jnp.int32)

    loads[0].wait()
    for k in range(SEND_MOST):
        pix[k, mp] = pixels_v[index[k]]
    loads[1].wait()
    line = lax.broadcasted_iota(jnp.int32, (32, 16), 0) // 8
    wanted = jnp.where(line == 0, index[0], jnp.where(line == 1, index[1], index[2]))
    chosen_rows = (lax.broadcasted_iota(jnp.int32, (32, 16), 1) == wanted).astype(F32).astype(BF16)
    tiles = diagonal(dot(chosen_rows, captions_v[...]))
    for k in range(SEND_MOST):
        cap_send[k] = tiles[8 * k : 8 * k + 8].astype(BF16)
    lane = lax.broadcasted_iota(jnp.int32, (8, 128), 1)
    goals = jnp.where(lane == 0, target[0], jnp.where(lane == 1, target[1], jnp.where(lane == 2, target[2], -1)))
    cap_send[3] = goals.astype(F32).astype(BF16)
    caps[dp] = cap_send[...]
    loads[3].wait()
    loads[5].wait()

    pl.semaphore_wait(barrier, n_dp - 1 + 3)

    mp_peers = ((right, 0), (left, 1), (opposite, 2))
    mp_sources = ((left, 0), (right, 1), (opposite, 2))
    for other, n in mp_peers:
        send(place.at[mp, core, y], px_s.at[n], px_r.at[n], (dp, other))

    def ring_send(piece, half, sends, receives, to_right, to_left):
        send(piece, sends.at[0], receives.at[0], to_right)
        send(piece, sends.at[1], receives.at[1], to_left)

    def ring_forward(from_left, from_right, half, sends, receives, to_right, to_left, lead=()):
        arrival(from_left, receives.at[0])
        first = from_left.at[pl.ds(0, half)]
        send(first, sends.at[2], receives.at[2], to_right)
        arrival(from_right, receives.at[1])
        second = from_right.at[pl.ds(half, half)]
        send(second, sends.at[3], receives.at[3], to_left)

    def ring_finish(far, half, receives):
        arrival(far.at[pl.ds(0, half)], receives.at[2])
        arrival(far.at[pl.ds(half, half)], receives.at[3])

    to_right, to_left = (dp, right), (dp, left)
    slice_rows = wo.shape[3]
    patch_rows = pix.shape[2]
    rows = n_mp * patch_rows

    def pix_send(k):
        ring_send(pix.at[k, mp], patch_rows // 2, pix_s.at[k], pix_r.at[k], to_right, to_left)

    def pix_forward(k):
        ring_forward(
            pix.at[k, left], pix.at[k, right], patch_rows // 2, pix_s.at[k], pix_r.at[k], to_right, to_left
        )

    ring_send(wo.at[mp, core, y], slice_rows // 2, wx_s, wx_r, to_right, to_left)
    pix_send(0)
    for source, n in mp_sources:
        arrival(place.at[source, core, y], px_r.at[n])
        for step in range(1, Y):
            send(
                place.at[source, core, y], py_s.at[n, step - 1], py_r.at[n, step - 1], (on_y(step), mp)
            )
    ring_forward(
        wo.at[left, core, y], wo.at[right, core, y], slice_rows // 2, wx_s, wx_r, to_right, to_left
    )
    pix_send(1)
    pix_forward(0)
    pix_send(2)
    for source, n in mp_sources:
        for step in range(1, Y):
            arrival(place.at[source, core, (y + Y - step) % Y], py_r.at[n, step - 1])
        send(place.at[source, core], pc_s.at[n], pc_r.at[n], (partner, mp))
    ring_finish(wo.at[opposite, core, y], slice_rows // 2, wx_r)
    for source, n in mp_sources:
        ring_send(
            wo.at[source, core, y], slice_rows // 2, wy_s.at[n], wy_r.at[n], (on_y(1), mp), (on_y(Y - 1), mp)
        )

    def cast_captions(step, carry):
        remote(cap_send, caps.at[dp], cap_s, cap_r, ((dp + step) % n_dp, mp)).start()
        return carry

    lax.fori_loop(1, n_dp, cast_captions, 0)
    pix_forward(1)
    loads[2].wait()
    for source, n in mp_sources:
        arrival(place.at[source, 1 - core], pc_r.at[n])
    loads[4].wait()

    gain0, gain1 = gains[0:1, :], gains[1:2, :]
    width = gains.shape[1]
    chunk_rows = 32

    def norm_into(k, gain):
        def one(part, carry):
            span = pl.ds(pl.multiple_of(part * chunk_rows, chunk_rows), chunk_rows)
            normed[span, :] = norm_rows(hid[k, span, :], gain).astype(BF16)
            return carry

        lax.fori_loop(0, rows // chunk_rows, one, 0, unroll=2)

    half_lane = lax.broadcasted_iota(jnp.int32, (rows, 128), 1) < HEAD_DIM
    ones = jnp.ones((rows, 128), BF16)
    to_both = (to_right, to_left)

    def attend(k, carry):
        ring_finish(pix.at[k, opposite], patch_rows // 2, pix_r.at[k])
        image = pix[k].reshape(rows, pix.shape[3])
        hid[k] = dot(image, patch_v[...]) + place[...].astype(F32).reshape(rows, width)
        norm_into(k, gain0)
        qkv[0] = (dot(normed[...], qkv_v[0]).astype(BF16) * BF16(HEAD_DIM ** (-0.5))).astype(BF16)
        qkv[1] = dot(normed[...], qkv_v[1]).astype(BF16)
        qkv[2] = dot(normed[...], qkv_v[2]).astype(BF16)
        for pair in range(qkv.shape[2] // 128):
            span = slice(pair * 128, pair * 128 + 128)
            query, keys, values = qkv[0, :, span], qkv[1, :, span], qkv[2, :, span]
            widened = jnp.concatenate([values, ones], axis=1)
            outs = []
            for head in range(2):
                mask = half_lane if head == 0 else jnp.logical_not(half_lane)
                mine = jnp.where(mask, query, jnp.zeros_like(query))
                scores = lax.dot_general(mine, keys, NT, preferred_element_type=F32)
                raised = jnp.exp(scores - jnp.max(scores, axis=1, keepdims=True)).astype(BF16)
                both = dot(raised, widened)
                outs.append(both[:, :128] / both[:, 128:])
            ctx[k, mp, :, span] = jnp.where(half_lane, outs[0], outs[1]).astype(BF16)
        for n, where in enumerate(to_both):
            remote(ctx.at[k, mp], ctx.at[k, mp], ctx_s.at[k, n], ctx_r.at[k, n], where).start()
        return carry

    attend(0, 0)
    pix_forward(2)
    for source, n in mp_sources:
        ring_forward(
            wo.at[source, core, y_down], wo.at[source, core, y_up], slice_rows // 2, wy_s.at[n], wy_r.at[n],
            (on_y(1), mp), (on_y(Y - 1), mp),
        )
    lax.fori_loop(1, SEND_MOST, attend, 0)
    for source, n in mp_sources:
        ring_finish(wo.at[source, core, y_far], slice_rows // 2, wy_r.at[n])
        send(wo.at[source, core], wc_s.at[n], wc_r.at[n], (partner, mp))
    half = rows // 2

    def ctx_forward(k):
        ring_forward(ctx.at[k, left], ctx.at[k, right], half, ctx_s.at[k], ctx_r.at[k], to_right, to_left)

    ctx_forward(0)

    others = caps.at[pl.ds(0, n_dp - 1)]
    pltpu.make_async_copy(others, others, cap_r).wait()
    flat = n_dp * 8
    goals = caps[:, 3].astype(F32).reshape(flat, 128)
    here = goals == dp.astype(F32)
    match = jnp.where(here, 1.0, 0.0)
    present = jnp.broadcast_to(jnp.sum(match, axis=1, keepdims=True), (flat, 128))
    row, column = (lax.broadcasted_iota(jnp.int32, (flat, flat), n) for n in range(2))
    earlier = jnp.where(jnp.logical_and(row // 8 > column // 8, column % 8 == 0), 1.0, 0.0).astype(BF16)
    order = dot(earlier, present.astype(BF16))
    lane = lax.broadcasted_iota(jnp.int32, (flat, 128), 1)
    line = lax.broadcasted_iota(jnp.int32, (flat, 128), 0)
    in_slot = jnp.where(order == (lane % 4).astype(F32), present, 0.0)
    spread = jnp.where(jnp.logical_and(line % 8 == lane // 16, lane % 16 < 12), in_slot, 0.0)
    picker[...] = spread.T.astype(BF16)
    filled = jnp.sum(jnp.max(in_slot.reshape(n_dp, 8, 128), axis=1), axis=0, keepdims=True)
    scale = 10.0 * jnp.exp(jnp.full((1, 128), loss_params[0], F32))
    shift = 2.0 * jnp.full((1, 128), loss_params[1], F32)
    for k in range(SEND_MOST):
        tiles = caps[:, k].astype(F32)
        caps_flat[pl.ds(k * flat, flat), :] = tiles.reshape(flat, 128).astype(BF16)
        square = jnp.sum(jnp.sum(tiles * tiles, axis=1), axis=1, keepdims=True)
        length = lax.rsqrt(square / width + EPS) * width ** (-0.5)
        weight_of[k] = length * scale
        column_of = jnp.sum(jnp.where(lane == k, match, 0.0), axis=1, keepdims=True)
        same = jnp.max((column_of * in_slot).reshape(n_dp, 8, 128), axis=1)
        alive = jnp.max(jnp.where(lane == k, goals, -1.0), axis=1, keepdims=True)
        alive = jnp.max(jnp.broadcast_to(alive, (flat, 128)).reshape(n_dp, 8, 128), axis=1)
        sign_of[k] = jnp.where(alive >= 0.0, 1.0 - 2.0 * same, 0.0)

    ctx_forward(1)
    ctx_forward(2)
    for source, n in mp_sources:
        arrival(wo.at[source, 1 - core], wc_r.at[n])
    loads[6].wait()

    def expand(k, carry):
        ring_finish(ctx.at[k, opposite], half, ctx_r.at[k])
        context = jnp.concatenate([ctx[k, source] for source in range(n_mp)], axis=1)
        hid[k] = hid[k] + dot(context, wo[...].reshape(width, width))
        norm_into(k, gain1)
        own = jnp.sum(hid[k, pl.ds(pl.multiple_of(mp * patch_rows, patch_rows), patch_rows), :], axis=0, keepdims=True)
        shared[mp, k] = diagonal(jnp.broadcast_to(own, (8, width)))
        block = 256
        for n in range(up_v.shape[1] // block):
            span = slice(n * block, n * block + block)
            units = jax.nn.gelu(dot(normed[...], up_v[:, span]))
            total = jnp.sum(units, axis=0, keepdims=True)
            summed[k, :, span] = jnp.broadcast_to(total, (8, block))
        return carry

    lax.fori_loop(0, SEND_MOST, expand, 0)

    loads[7].wait()
    totals = summed[...].reshape(SEND_MOST * 8, width)
    high = totals.astype(BF16)
    low = (totals - high.astype(F32)).astype(BF16)
    down = dot(high, down_v[...]) + dot(low, down_v[...])
    shared[mp] = shared[mp] + diagonal(down).reshape(SEND_MOST, 8, 128)
    for other, n in mp_peers:
        send(shared.at[mp], ar_s.at[n], ar_r.at[n], (dp, other))
    for source, n in mp_sources:
        arrival(shared.at[source], ar_r.at[n])
    pooled = (shared[0] + shared[1]) + (shared[2] + shared[3])
    pooled = pooled / rows

    def mean_of(tiles):
        return jnp.sum(jnp.sum(tiles, axis=2, keepdims=True), axis=1, keepdims=True) / width

    centred = pooled - mean_of(pooled)
    gain2 = diagonal(jnp.broadcast_to(gains[2:3, :], (8, width)))
    ready = centred * lax.rsqrt(mean_of(centred * centred) + EPS) * gain2[None]
    goal_of = lax.broadcasted_iota(jnp.int32, (n_dp, 8, 128), 0)
    outgoing = jnp.zeros((n_dp, 8, 128), F32)
    for k in range(SEND_MOST):
        outgoing = jnp.where(goal_of == target[k], ready[k][None], outgoing)
    out_send[...] = outgoing.astype(BF16)
    arrived[dp] = out_send[dp]

    def deliver(step, carry):
        there = (dp + step) % n_dp
        remote(out_send.at[there], arrived.at[dp], out_s, out_r, (there, mp)).start()
        return carry

    lax.fori_loop(1, n_dp, deliver, 0)
    loads[8].wait()
    others = arrived.at[pl.ds(0, n_dp - 1)]
    pltpu.make_async_copy(others, others, out_r).wait()

    slots = dot(picker[...], arrived[...].astype(F32).reshape(flat, 128).astype(BF16)).astype(BF16)
    slots = jnp.concatenate([slots[n * 16 : n * 16 + 16] for n in range(8)], axis=1)
    embedded = dot(slots, embedding_v[...])
    embedded_out[...] = embedded[:RECV_MOST]
    unit = embedded * (lax.rsqrt(jnp.mean(embedded * embedded, axis=1, keepdims=True) + EPS) * width ** (-0.5))
    first = unit.astype(BF16).astype(F32)
    rest = unit - first
    second = rest.astype(BF16).astype(F32)
    line = lax.broadcasted_iota(jnp.int32, unit.shape, 0)
    parts = jnp.where(line < 4, first, jnp.where(line < 8, second, jnp.where(line < 12, rest - second, 0.0)))
    parts = parts.astype(BF16)
    parts = jnp.concatenate([parts[:, n * 128 : n * 128 + 128] for n in range(8)], axis=0)
    products = lax.dot_general(caps_flat[...], parts, NT, preferred_element_type=F32)
    line = lax.broadcasted_iota(jnp.int32, (SEND_MOST * flat, 128), 0)
    lane = lax.broadcasted_iota(jnp.int32, (SEND_MOST * flat, 128), 1)
    products = jnp.where(line % 8 == lane // 16, products, 0.0).reshape(SEND_MOST * n_dp, 8, 128)
    products = jnp.sum(products, axis=1)
    for step in (64, 32, 16, 8, 4):
        products = products + pltpu.roll(products, step, 1)
    weights = weight_of[...].reshape(SEND_MOST * n_dp, 128)
    signs = sign_of[...].reshape(SEND_MOST * n_dp, 128)
    terms = signs * (products * weights + shift)
    terms = jnp.maximum(terms, 0.0) + jnp.log1p(jnp.exp(-jnp.abs(terms)))
    terms = jnp.where(signs == 0.0, 0.0, terms)
    losses = jnp.sum(terms, axis=0, keepdims=True) / float(n_dp * SEL_DEV)
    losses_out[...] = jnp.where(filled > 0.0, losses, 0.0)

    for src, ref, sends, receives, where in pending:
        remote(src, ref, sends, receives, where).wait_send()
    for k in range(SEND_MOST):
        for n, where in enumerate(to_both):
            remote(ctx.at[k, mp], ctx.at[k, mp], ctx_s.at[k, n], ctx_r.at[k, n], where).wait_send()
    others = caps.at[pl.ds(0, n_dp - 1)]
    pltpu.make_async_copy(others, others, cap_s).wait()
    others = arrived.at[pl.ds(0, n_dp - 1)]
    pltpu.make_async_copy(others, others, out_s).wait()


def per_device(
    pixels, selection, destination, patch_weight, position, query_key_value, output_weight, up_weight,
    down_weight, norm_gains, embedding_weight, caption_vectors, loss_params,
):
    n_dp, n_mp = lax.axis_size("dp"), lax.axis_size("mp")
    width, units = up_weight.shape
    share = query_key_value.shape[2]
    patch_rows, values = pixels.shape[1:]
    rows = n_mp * patch_rows
    place_rows = position.shape[0] // (Y * CORES)
    slice_rows = output_weight.shape[0] // (Y * CORES)
    position = position.reshape(CORES, Y, place_rows, width)
    output_weight = output_weight.reshape(CORES, Y, slice_rows, width)
    smem = pl.BlockSpec(memory_space=pltpu.SMEM)
    vmem = pl.BlockSpec(memory_space=pltpu.VMEM)
    far = pl.BlockSpec(memory_space=pl.ANY)
    dma = pltpu.SemaphoreType.DMA
    n = SEND_MOST
    scratch = [
        pltpu.VMEM(pixels.shape, BF16), pltpu.VMEM(patch_weight.shape, BF16),
        pltpu.VMEM(query_key_value.shape, BF16), pltpu.VMEM(up_weight.shape, BF16),
        pltpu.VMEM(down_weight.shape, BF16), pltpu.VMEM(embedding_weight.shape, BF16),
        pltpu.VMEM(caption_vectors.shape, BF16),
        pltpu.VMEM((n, n_mp, patch_rows, values), BF16),
        pltpu.VMEM((n_mp, CORES, Y, place_rows, width), BF16),
        pltpu.VMEM((n_mp, CORES, Y, slice_rows, width), BF16),
        pltpu.VMEM((n, rows, width), F32), pltpu.VMEM((rows, width), BF16),
        pltpu.VMEM((3, rows, share), BF16), pltpu.VMEM((n, n_mp, rows, share), BF16),
        pltpu.VMEM((n + 1, 8, 128), BF16), pltpu.VMEM((n_dp, n + 1, 8, 128), BF16),
        pltpu.VMEM((n * n_dp * 8, 128), BF16), pltpu.VMEM((n, 8, units), F32),
        pltpu.VMEM((n_mp, n, 8, 128), F32),
        pltpu.VMEM((n_dp, 8, 128), BF16), pltpu.VMEM((n_dp, 8, 128), BF16),
        pltpu.VMEM((128, n_dp * 8), BF16), pltpu.VMEM((n, n_dp, 128), F32), pltpu.VMEM((n, n_dp, 128), F32),
        dma((9,)), dma((n, 4)), dma((n, 4)), dma((3,)), dma((3,)), dma((3, 3)), dma((3, 3)), dma((3,)), dma((3,)),
        dma((4,)), dma((4,)), dma((3, 4)), dma((3, 4)), dma((3,)), dma((3,)),
        dma((n, 4)), dma((n, 4)), dma((3,)), dma((3,)), dma, dma, dma, dma,
    ]
    embedded, losses = pl.pallas_call(
        functools.partial(body, n_dp, n_mp),
        out_shape=(
            jax.ShapeDtypeStruct((RECV_MOST, width), F32),
            jax.ShapeDtypeStruct((1, 128), F32),
        ),
        in_specs=[smem, smem, smem, far, far, far, far, far, far, far, vmem, far, far],
        out_specs=(vmem, vmem),
        scratch_shapes=scratch,
        name="learner",
        compiler_params=pltpu.CompilerParams(
            collective_id=0, has_side_effects=True, vmem_limit_bytes=60 * 1024 * 1024
        ),
    )(
        selection, destination, loss_params, pixels, patch_weight, position, query_key_value, output_weight,
        up_weight, down_weight, norm_gains, embedding_weight, caption_vectors,
    )
    return embedded, losses[0, :RECV_MOST]


def solution(mesh):
    in_specs = (
        P("dp", "mp", None), P("dp"), P("dp"), P(), P("mp", None), P(None, None, "mp"), P("mp", None),
        P(None, "mp"), P("mp", None), P(), P(), P("dp", None), P(),
    )
    out_specs = (P("dp", None), P("dp"))
    return jax.shard_map(per_device, mesh=mesh, in_specs=in_specs, out_specs=out_specs, check_vma=False)
```

```python
import functools

import jax
import jax.numpy as jnp
from jax import lax
from jax.experimental import pallas as pl
from jax.experimental.pallas import tpu as pltpu
from jax.sharding import PartitionSpec as P

EPS = 1e-06
SEND_MOST = 3
RECV_MOST = 4
SEL_DEV = 2
HEAD_DIM = 64
Y, CORES = 4, 2
F32, BF16 = jnp.float32, jnp.bfloat16
NT = (((1,), (1,)), ((), ()))


def norm_rows(values, gain):
    center = jnp.mean(values, axis=-1, keepdims=True)
    centred = values - center
    spread = jnp.mean(centred * centred, axis=-1, keepdims=True)
    return centred * lax.rsqrt(spread + EPS) * gain


def diagonal(rows):
    count = rows.shape[0]
    line = lax.broadcasted_iota(jnp.int32, (count, 128), 0) % 8
    out = jnp.zeros((count, 128), rows.dtype)
    for chunk in range(8):
        out = jnp.where(line == chunk, rows[:, chunk * 128 : (chunk + 1) * 128], out)
    return out


def dot(a, b):
    return jnp.dot(a, b, preferred_element_type=F32)


def body(
    n_dp, n_mp,
    selection_h, destination_h, loss_params_h, pixels, patch_weight, position, query_key_value, output_weight,
    up_weight, down_weight, gains_h, embedding_weight, captions,
    embedded_out, losses_out,
    selection, destination, loss_params, gains, pixels_v, patch_v, qkv_v, up_v, down_v, embedding_v, captions_v,
    pix, place, wo, hid, normed, qkv, ctx, cap_send, caps, caps_flat, summed, shared,
    out_send, arrived, picker, sign_of, weight_of,
    local, pix_s, pix_r, px_s, px_r, py_s, py_r, pc_s, pc_r, wx_s, wx_r, wy_s, wy_r, wc_s, wc_r,
    ctx_s, ctx_r, ar_s, ar_r, cy_s, cy_r, cz_s, cz_r, cc_s, cc_r, out_s, out_r, entered,
):
    dp, mp = lax.axis_index("dp"), lax.axis_index("mp")
    right, left, opposite = (mp + 1) % n_mp, (mp + n_mp - 1) % n_mp, (mp + 2) % n_mp
    core, y, z = dp % CORES, (dp // CORES) % Y, dp // (CORES * Y)

    def on_y(step):
        return (z * Y + (y + step) % Y) * CORES + core

    partner = dp + 1 - 2 * core

    def remote(src, dst, sends, receives, where):
        return pltpu.make_async_remote_copy(
            src_ref=src, dst_ref=dst, send_sem=sends, recv_sem=receives, device_id=where,
            device_id_type=pl.DeviceIdType.MESH,
        )

    draining = []

    def arrival(ref, receives):
        if draining:
            return
        remote(ref, ref, receives, receives, (dp, right)).wait_recv()

    def send(ref, sends, receives, where):
        copy = remote(ref, ref, sends, receives, where)
        if draining:
            copy.wait_send()
        else:
            copy.start()

    barrier = pltpu.get_barrier_semaphore()

    def greet(where):
        pl.semaphore_signal(barrier, inc=1, device_id=where, device_id_type=pl.DeviceIdType.MESH)

    def far_first(act):
        act(dp, n_dp // 2)

        def both(step, carry):
            act(dp, n_dp // 2 - step)
            act(dp, n_dp // 2 + step)
            return carry

        lax.fori_loop(1, n_dp // 2, both, 0)

    loads = [
        (selection_h, selection), (destination_h, destination), (pixels, pixels_v), (captions, captions_v),
        (position, place.at[mp]), (output_weight, wo.at[mp]), (patch_weight, patch_v), (gains_h, gains),
        (query_key_value, qkv_v), (loss_params_h, loss_params), (up_weight, up_v), (down_weight, down_v),
        (embedding_weight, embedding_v),
    ]
    loads = [pltpu.make_async_copy(a, b, local.at[n]) for n, (a, b) in enumerate(loads)]
    for load in loads[:4]:
        load.start()
    near = [(dp, opposite), (on_y(2), mp), (dp, right), (dp, left), (on_y(1), mp), (on_y(Y - 1), mp), (partner, mp)]
    n_z = n_dp // (Y * CORES)
    z_near = [((dp + step * Y * CORES) % n_dp, mp) for step in (1, n_z - 1)] if n_z > 1 else []
    for where in near + z_near:
        greet(where)
    for load in loads[4:]:
        load.start()

    loads[0].wait()
    loads[1].wait()
    index = [jnp.int32(0)] * SEND_MOST
    target = [jnp.int32(-1)] * SEND_MOST
    count = jnp.int32(0)
    for example in range(selection.shape[0]):
        chosen = selection[example] > 0
        goal = destination[example]
        for k in range(SEND_MOST):
            hit = jnp.logical_and(chosen, count == k)
            index[k] = jnp.where(hit, example, index[k])
            target[k] = jnp.where(hit, goal, target[k])
        count = count + chosen.astype(jnp.int32)

    loads[2].wait()
    for k in range(SEND_MOST):
        pix[k, mp] = pixels_v[index[k]]
    loads[3].wait()
    line = lax.broadcasted_iota(jnp.int32, (32, 16), 0) // 8
    wanted = jnp.where(line == 0, index[0], jnp.where(line == 1, index[1], index[2]))
    chosen_rows = (lax.broadcasted_iota(jnp.int32, (32, 16), 1) == wanted).astype(F32).astype(BF16)
    tiles = diagonal(dot(chosen_rows, captions_v[...]))
    for k in range(SEND_MOST):
        cap_send[k] = tiles[8 * k : 8 * k + 8].astype(BF16)
    lane = lax.broadcasted_iota(jnp.int32, (8, 128), 1)
    goals = jnp.where(lane == 0, target[0], jnp.where(lane == 1, target[1], jnp.where(lane == 2, target[2], -1)))
    cap_send[3] = goals.astype(F32).astype(BF16)
    caps[core, z, y] = cap_send[...]
    loads[4].wait()
    loads[5].wait()

    pl.semaphore_wait(barrier, len(near + z_near))

    def tell(step):
        for where in z_near if step else [(on_y(n), mp) for n in range(1, Y)]:
            pl.semaphore_signal(entered.at[step], inc=1, device_id=where, device_id_type=pl.DeviceIdType.MESH)

    def told(step):
        pl.semaphore_wait(entered.at[step], len(z_near) if step else Y - 1)

    tell(0)

    mp_peers = ((right, 0), (left, 1), (opposite, 2))
    mp_sources = ((left, 0), (right, 1), (opposite, 2))

    def halves(piece):
        half = piece.shape[0] // 2
        return piece.at[pl.ds(0, half)], piece.at[pl.ds(half, half)]

    def ring_send(piece, sends, receives, to_right, to_left):
        first, second = halves(piece)
        send(first, sends.at[0], receives.at[0], to_right)
        send(second, sends.at[2], receives.at[2], to_left)
        send(second, sends.at[1], receives.at[1], to_right)
        send(first, sends.at[3], receives.at[3], to_left)

    def ring_forward(from_left, from_right, sends, receives, to_right, to_left):
        first, second = halves(from_left)[0], halves(from_right)[1]
        arrival(first, receives.at[0])
        send(first, sends.at[4], receives.at[4], to_right)
        arrival(second, receives.at[2])
        send(second, sends.at[5], receives.at[5], to_left)

    def ring_finish(from_left, from_right, far, receives):
        arrival(halves(from_left)[1], receives.at[1])
        arrival(halves(from_right)[0], receives.at[3])
        arrival(halves(far)[0], receives.at[4])
        arrival(halves(far)[1], receives.at[5])

    to_right, to_left = (dp, right), (dp, left)
    patch_rows = pix.shape[2]
    rows = n_mp * patch_rows

    def pix_send(k):
        ring_send(pix.at[k, mp], pix_s.at[k], pix_r.at[k], to_right, to_left)

    def pix_forward(k):
        ring_forward(
            pix.at[k, left], pix.at[k, right], pix_s.at[k], pix_r.at[k], to_right, to_left
        )

    def place_x():
        for other, n in mp_peers:
            send(place.at[mp, core, y], px_s.at[n], px_r.at[n], (dp, other))

    def place_y():
        for source, n in mp_sources:
            arrival(place.at[source, core, y], px_r.at[n])
            for step in range(1, Y):
                send(
                    place.at[source, core, y], py_s.at[n, step - 1], py_r.at[n, step - 1], (on_y(step), mp)
                )

    def place_core():
        for source, n in mp_sources:
            for step in range(1, Y):
                arrival(place.at[source, core, (y + Y - step) % Y], py_r.at[n, step - 1])
            send(place.at[source, core], pc_s.at[n], pc_r.at[n], (partner, mp))

    def wo_x():
        ring_send(wo.at[mp, core, y], wx_s, wx_r, to_right, to_left)

    def wo_x_forward():
        ring_forward(wo.at[left, core, y], wo.at[right, core, y], wx_s, wx_r, to_right, to_left)

    def wo_y():
        ring_finish(wo.at[left, core, y], wo.at[right, core, y], wo.at[opposite, core, y], wx_r)
        for source, n in mp_sources:
            for step in (2, 1, 3):
                send(wo.at[source, core, y], wy_s.at[n, step - 1], wy_r.at[n, step - 1], (on_y(step), mp))

    def wo_core():
        for source, n in mp_sources:
            for step in range(1, Y):
                arrival(wo.at[source, core, (y + Y - step) % Y], wy_r.at[n, step - 1])
            send(wo.at[source, core], wc_s.at[n], wc_r.at[n], (partner, mp))

    def caps_y():
        for step in range(1, Y):
            send(caps.at[core, z, y], cy_s.at[step - 1], cy_r.at[step - 1], (on_y(step), mp))

    def caps_z():
        for step in range(1, Y):
            arrival(caps.at[core, z, (y + Y - step) % Y], cy_r.at[step - 1])
        for step in range(1, n_z):
            there = ((((z + step) % n_z) * Y + y) * CORES + core, mp)
            send(caps.at[core, z], cz_s.at[step - 1], cz_r.at[step - 1], there)

    def caps_core():
        for step in range(1, n_z):
            arrival(caps.at[core, (z + n_z - step) % n_z], cz_r.at[step - 1])
        send(caps.at[core], cc_s, cc_r, (partner, mp))

    place_x()
    pix_send(0)
    wo_x()
    caps_y()
    place_y()
    pix_send(1)
    told(0)
    tell(1)
    pix_forward(0)
    wo_x_forward()
    pix_send(2)
    told(1)
    tell(2)
    place_core()
    told(2)
    tell(3)
    pix_forward(1)
    loads[6].wait()
    loads[7].wait()
    loads[8].wait()

    gain0, gain1 = gains[0:1, :], gains[1:2, :]
    width = gains.shape[1]
    chunk_rows = 32

    def norm_into(k, gain):
        def one(part, carry):
            span = pl.ds(pl.multiple_of(part * chunk_rows, chunk_rows), chunk_rows)
            normed[span, :] = norm_rows(hid[k, span, :], gain).astype(BF16)
            return carry

        lax.fori_loop(0, rows // chunk_rows, one, 0, unroll=2)

    half_lane = lax.broadcasted_iota(jnp.int32, (rows, 128), 1) < HEAD_DIM
    ones = jnp.ones((rows, 128), BF16)

    def ctx_send(k):
        ring_send(ctx.at[k, mp], ctx_s.at[k], ctx_r.at[k], to_right, to_left)

    def ctx_forward(k):
        ring_forward(ctx.at[k, left], ctx.at[k, right], ctx_s.at[k], ctx_r.at[k], to_right, to_left)

    def attend(k, carry):
        ring_finish(pix.at[k, left], pix.at[k, right], pix.at[k, opposite], pix_r.at[k])
        image = pix[k].reshape(rows, pix.shape[3])
        hid[k] = dot(image, patch_v[...])

        @pl.when(k == 0)
        def _():
            for source, n in mp_sources:
                arrival(place.at[source, 1 - core], pc_r.at[n])
            told(3)
            tell(4)
            wo_y()

        hid[k] = hid[k] + place[...].astype(F32).reshape(rows, width)
        norm_into(k, gain0)
        qkv[0] = (dot(normed[...], qkv_v[0]).astype(BF16) * BF16(HEAD_DIM ** (-0.5))).astype(BF16)
        qkv[1] = dot(normed[...], qkv_v[1]).astype(BF16)
        qkv[2] = dot(normed[...], qkv_v[2]).astype(BF16)
        @pl.when(k == 2)
        def _():
            caps_core()

        for pair in range(qkv.shape[2] // 128):
            span = slice(pair * 128, pair * 128 + 128)
            query, keys, values = qkv[0, :, span], qkv[1, :, span], qkv[2, :, span]
            widened = jnp.concatenate([values, ones], axis=1)
            outs = []
            for head in range(2):
                mask = half_lane if head == 0 else jnp.logical_not(half_lane)
                mine = jnp.where(mask, query, jnp.zeros_like(query))
                scores = lax.dot_general(mine, keys, NT, preferred_element_type=F32)
                raised = jnp.exp(scores - jnp.max(scores, axis=1, keepdims=True)).astype(BF16)
                both = dot(raised, widened)
                outs.append(both[:, :128] / both[:, 128:])
            ctx[k, mp, :, span] = jnp.where(half_lane, outs[0], outs[1]).astype(BF16)

        ctx_send(k)

        @pl.when(k == 0)
        def _():
            pix_forward(2)
            told(4)
            caps_z()

        @pl.when(k == 1)
        def _():
            ctx_forward(0)

        return carry

    lax.fori_loop(0, SEND_MOST, attend, 0)
    ctx_forward(1)
    wo_core()

    arrival(caps.at[1 - core], cc_r)
    caps_all = caps[...].reshape(n_dp, SEND_MOST + 1, 8, 128)
    flat = n_dp * 8
    goals = caps_all[:, 3].astype(F32).reshape(flat, 128)
    here = goals == dp.astype(F32)
    match = jnp.where(here, 1.0, 0.0)
    present = jnp.broadcast_to(jnp.sum(match, axis=1, keepdims=True), (flat, 128))
    row, column = (lax.broadcasted_iota(jnp.int32, (flat, flat), n) for n in range(2))
    row_dp, column_dp = (n // 8 % (n_dp // CORES) * CORES + n // 8 // (n_dp // CORES) for n in (row, column))
    earlier = jnp.where(jnp.logical_and(row_dp > column_dp, column % 8 == 0), 1.0, 0.0).astype(BF16)
    order = dot(earlier, present.astype(BF16))
    lane = lax.broadcasted_iota(jnp.int32, (flat, 128), 1)
    line = lax.broadcasted_iota(jnp.int32, (flat, 128), 0)
    in_slot = jnp.where(order == (lane % 4).astype(F32), present, 0.0)
    spread = jnp.where(jnp.logical_and(line % 8 == lane // 16, lane % 16 < 12), in_slot, 0.0)
    picker[...] = spread.T.astype(BF16)
    filled = jnp.sum(jnp.max(in_slot.reshape(n_dp, 8, 128), axis=1), axis=0, keepdims=True)
    loads[9].wait()
    scale = 10.0 * jnp.exp(jnp.full((1, 128), loss_params[0], F32))
    shift = 2.0 * jnp.full((1, 128), loss_params[1], F32)
    for k in range(SEND_MOST):
        tiles = caps_all[:, k].astype(F32)
        caps_flat[pl.ds(k * flat, flat), :] = tiles.reshape(flat, 128).astype(BF16)
        square = jnp.sum(jnp.sum(tiles * tiles, axis=1), axis=1, keepdims=True)
        length = lax.rsqrt(square / width + EPS) * width ** (-0.5)
        weight_of[k] = length * scale
        column_of = jnp.sum(jnp.where(lane == k, match, 0.0), axis=1, keepdims=True)
        same = jnp.max((column_of * in_slot).reshape(n_dp, 8, 128), axis=1)
        alive = jnp.max(jnp.where(lane == k, goals, -1.0), axis=1, keepdims=True)
        alive = jnp.max(jnp.broadcast_to(alive, (flat, 128)).reshape(n_dp, 8, 128), axis=1)
        sign_of[k] = jnp.where(alive >= 0.0, 1.0 - 2.0 * same, 0.0)

    for source, n in mp_sources:
        arrival(wo.at[source, 1 - core], wc_r.at[n])
    loads[10].wait()

    def expand(k, carry):
        ring_finish(ctx.at[k, left], ctx.at[k, right], ctx.at[k, opposite], ctx_r.at[k])
        context = jnp.concatenate([ctx[k, source] for source in range(n_mp)], axis=1)
        hid[k] = hid[k] + dot(context, wo[...].reshape(width, width))
        norm_into(k, gain1)
        own = jnp.sum(hid[k, pl.ds(pl.multiple_of(mp * patch_rows, patch_rows), patch_rows), :], axis=0, keepdims=True)
        shared[mp, k] = diagonal(jnp.broadcast_to(own, (8, width)))
        block = 256
        for n in range(up_v.shape[1] // block):
            span = slice(n * block, n * block + block)
            units = jax.nn.gelu(dot(normed[...], up_v[:, span]))
            total = jnp.sum(units, axis=0, keepdims=True)
            summed[k, :, span] = jnp.broadcast_to(total, (8, block))

        @pl.when(k == 0)
        def _():
            ctx_forward(2)

        return carry

    lax.fori_loop(0, SEND_MOST, expand, 0)

    loads[11].wait()
    totals = summed[...].reshape(SEND_MOST * 8, width)
    high = totals.astype(BF16)
    low = (totals - high.astype(F32)).astype(BF16)
    down = dot(jnp.concatenate([high, low], axis=0), down_v[...])
    down = down[: SEND_MOST * 8] + down[SEND_MOST * 8 :]
    shared[mp] = shared[mp] + diagonal(down).reshape(SEND_MOST, 8, 128)

    def share():
        for other, n in mp_peers:
            send(shared.at[mp], ar_s.at[n], ar_r.at[n], (dp, other))

    share()
    for source, n in mp_sources:
        arrival(shared.at[source], ar_r.at[n])
    pooled = (shared[0] + shared[1]) + (shared[2] + shared[3])
    pooled = pooled / rows

    def mean_of(tiles):
        return jnp.sum(jnp.sum(tiles, axis=2, keepdims=True), axis=1, keepdims=True) / width

    centred = pooled - mean_of(pooled)
    gain2 = diagonal(jnp.broadcast_to(gains[2:3, :], (8, width)))
    ready = centred * lax.rsqrt(mean_of(centred * centred) + EPS) * gain2[None]
    goal_of = lax.broadcasted_iota(jnp.int32, (n_dp, 8, 128), 0)
    outgoing = jnp.zeros((n_dp, 8, 128), F32)
    for k in range(SEND_MOST):
        outgoing = jnp.where(goal_of == target[k], ready[k][None], outgoing)
    out_send[...] = outgoing.astype(BF16)
    spot = core * (n_dp // CORES) + dp // CORES
    arrived[spot] = out_send[dp]

    def deliver(me, step):
        there = (me + step) % n_dp
        remote(out_send.at[there], arrived.at[spot], out_s, out_r, (there, mp)).start()

    far_first(deliver)
    loads[12].wait()
    others = arrived.at[pl.ds(0, n_dp - 1)]
    pltpu.make_async_copy(others, others, out_r).wait()

    slots = dot(picker[...], arrived[...].astype(F32).reshape(flat, 128).astype(BF16)).astype(BF16)
    slots = jnp.concatenate([slots[n * 16 : n * 16 + 16] for n in range(8)], axis=1)
    embedded = dot(slots, embedding_v[...])
    embedded_out[...] = embedded[:RECV_MOST]
    unit = embedded * (lax.rsqrt(jnp.mean(embedded * embedded, axis=1, keepdims=True) + EPS) * width ** (-0.5))
    first = unit.astype(BF16).astype(F32)
    rest = unit - first
    second = rest.astype(BF16).astype(F32)
    line = lax.broadcasted_iota(jnp.int32, unit.shape, 0)
    parts = jnp.where(line < 4, first, jnp.where(line < 8, second, jnp.where(line < 12, rest - second, 0.0)))
    parts = parts.astype(BF16)
    parts = jnp.concatenate([parts[:, n * 128 : n * 128 + 128] for n in range(8)], axis=0)
    products = lax.dot_general(caps_flat[...], parts, NT, preferred_element_type=F32)
    line = lax.broadcasted_iota(jnp.int32, (SEND_MOST * flat, 128), 0)
    lane = lax.broadcasted_iota(jnp.int32, (SEND_MOST * flat, 128), 1)
    products = jnp.where(line % 8 == lane // 16, products, 0.0).reshape(SEND_MOST * n_dp, 8, 128)
    products = jnp.sum(products, axis=1)
    for step in (64, 32, 16, 8, 4):
        products = products + pltpu.roll(products, step, 1)
    weights = weight_of[...].reshape(SEND_MOST * n_dp, 128)
    signs = sign_of[...].reshape(SEND_MOST * n_dp, 128)
    terms = signs * (products * weights + shift)
    terms = jnp.maximum(terms, 0.0) + jnp.log1p(jnp.exp(-jnp.abs(terms)))
    terms = jnp.where(signs == 0.0, 0.0, terms)
    losses = jnp.sum(terms, axis=0, keepdims=True) / float(n_dp * SEL_DEV)
    losses_out[...] = jnp.where(filled > 0.0, losses, 0.0)

    draining.append(True)
    for act in (place_x, place_y, place_core, wo_x, wo_x_forward, wo_y, wo_core, caps_y, caps_z, caps_core, share):
        act()
    for k in range(SEND_MOST):
        for act in (pix_send, pix_forward, ctx_send, ctx_forward):
            act(k)
    others = arrived.at[pl.ds(0, n_dp - 1)]
    pltpu.make_async_copy(others, others, out_s).wait()


def hand_over(embedded, losses, embedded_out, losses_out):
    embedded_out[...] = embedded[...]
    losses_out[...] = losses[0, :RECV_MOST]


def per_device(
    pixels, selection, destination, patch_weight, position, query_key_value, output_weight, up_weight,
    down_weight, norm_gains, embedding_weight, caption_vectors, loss_params,
):
    n_dp, n_mp = lax.axis_size("dp"), lax.axis_size("mp")
    width, units = up_weight.shape
    share = query_key_value.shape[2]
    patch_rows, values = pixels.shape[1:]
    rows = n_mp * patch_rows
    place_rows = position.shape[0] // (Y * CORES)
    slice_rows = output_weight.shape[0] // (Y * CORES)
    position = position.reshape(CORES, Y, place_rows, width)
    output_weight = output_weight.reshape(CORES, Y, slice_rows, width)
    vmem = pl.BlockSpec(memory_space=pltpu.VMEM)
    far = pl.BlockSpec(memory_space=pl.ANY)
    dma = pltpu.SemaphoreType.DMA
    n = SEND_MOST
    scratch = [
        pltpu.SMEM(selection.shape, jnp.int32), pltpu.SMEM(destination.shape, jnp.int32),
        pltpu.SMEM(loss_params.shape, F32), pltpu.VMEM(norm_gains.shape, F32),
        pltpu.VMEM(pixels.shape, BF16), pltpu.VMEM(patch_weight.shape, BF16),
        pltpu.VMEM(query_key_value.shape, BF16), pltpu.VMEM(up_weight.shape, BF16),
        pltpu.VMEM(down_weight.shape, BF16), pltpu.VMEM(embedding_weight.shape, BF16),
        pltpu.VMEM(caption_vectors.shape, BF16),
        pltpu.VMEM((n, n_mp, patch_rows, values), BF16),
        pltpu.VMEM((n_mp, CORES, Y, place_rows, width), BF16),
        pltpu.VMEM((n_mp, CORES, Y, slice_rows, width), BF16),
        pltpu.VMEM((n, rows, width), F32), pltpu.VMEM((rows, width), BF16),
        pltpu.VMEM((3, rows, share), BF16), pltpu.VMEM((n, n_mp, rows, share), BF16),
        pltpu.VMEM((n + 1, 8, 128), BF16), pltpu.VMEM((CORES, n_dp // (CORES * Y), Y, n + 1, 8, 128), BF16),
        pltpu.VMEM((n * n_dp * 8, 128), BF16), pltpu.VMEM((n, 8, units), F32),
        pltpu.VMEM((n_mp, n, 8, 128), F32),
        pltpu.VMEM((n_dp, 8, 128), BF16), pltpu.VMEM((n_dp, 8, 128), BF16),
        pltpu.VMEM((128, n_dp * 8), BF16), pltpu.VMEM((n, n_dp, 128), F32), pltpu.VMEM((n, n_dp, 128), F32),
        dma((13,)), dma((n, 6)), dma((n, 6)), dma((3,)), dma((3,)), dma((3, 3)), dma((3, 3)), dma((3,)), dma((3,)),
        dma((6,)), dma((6,)), dma((3, 3)), dma((3, 3)), dma((3,)), dma((3,)),
        dma((n, 6)), dma((n, 6)), dma((3,)), dma((3,)), dma((3,)), dma((3,)),
        dma((7,)), dma((7,)), dma, dma, dma, dma, pltpu.SemaphoreType.REGULAR((5,)),
    ]
    embedded, losses = pl.pallas_call(
        functools.partial(body, n_dp, n_mp),
        out_shape=(
            jax.ShapeDtypeStruct((RECV_MOST, width), F32),
            jax.ShapeDtypeStruct((1, 128), F32),
        ),
        in_specs=[far] * 13,
        out_specs=(vmem, vmem),
        scratch_shapes=scratch,
        name="learner",
        compiler_params=pltpu.CompilerParams(
            collective_id=0, has_side_effects=True, vmem_limit_bytes=60 * 1024 * 1024
        ),
    )(
        selection, destination, loss_params, pixels, patch_weight, position, query_key_value, output_weight,
        up_weight, down_weight, norm_gains, embedding_weight, caption_vectors,
    )
    return pl.pallas_call(
        hand_over,
        out_shape=(jax.ShapeDtypeStruct((RECV_MOST, width), F32), jax.ShapeDtypeStruct((RECV_MOST,), F32)),
        name="hand_over",
    )(embedded, losses)


def solution(mesh):
    in_specs = (
        P("dp", "mp", None), P("dp"), P("dp"), P(), P("mp", None), P(None, None, "mp"), P("mp", None),
        P(None, "mp"), P("mp", None), P(), P(), P("dp", None), P(),
    )
    out_specs = (P("dp", None), P("dp"))
    return jax.shard_map(per_device, mesh=mesh, in_specs=in_specs, out_specs=out_specs, check_vma=False)
```

```python
import functools

import jax
import jax.numpy as jnp
from jax import lax
from jax.experimental import pallas as pl
from jax.experimental.pallas import tpu as pltpu
from jax.sharding import PartitionSpec as P

EPS = 1e-06
SEND_MOST = 3
RECV_MOST = 4
SEL_DEV = 2
HEAD_DIM = 64
Y, CORES = 4, 2
F32, BF16 = jnp.float32, jnp.bfloat16
NT = (((1,), (1,)), ((), ()))


def norm_rows(values, gain):
    center = jnp.mean(values, axis=-1, keepdims=True)
    centred = values - center
    spread = jnp.mean(centred * centred, axis=-1, keepdims=True)
    return centred * lax.rsqrt(spread + EPS) * gain


def diagonal(rows):
    count = rows.shape[0]
    line = lax.broadcasted_iota(jnp.int32, (count, 128), 0) % 8
    out = jnp.zeros((count, 128), rows.dtype)
    for chunk in range(8):
        out = jnp.where(line == chunk, rows[:, chunk * 128 : (chunk + 1) * 128], out)
    return out


def dot(a, b):
    return jnp.dot(a, b, preferred_element_type=F32)


def body(
    n_dp, n_mp,
    selection_h, destination_h, loss_params_h, pixels, patch_weight, position, query_key_value, output_weight,
    up_weight, down_weight, gains_h, embedding_weight, captions,
    embedded_out, losses_out,
    selection, destination, loss_params, gains, pixels_v, patch_v, qkv_v, up_v, down_v, embedding_v, captions_v,
    pix, place, wo, hid, normed, qkv, ctx, cap_send, caps, caps_flat, summed, shared,
    out_send, arrived, picker, sign_of, weight_of,
    local, pix_s, pix_r, px_s, px_r, py_s, py_r, pc_s, pc_r, wx_s, wx_r, wy_s, wy_r, wc_s, wc_r,
    ctx_s, ctx_r, ar_s, ar_r, cy_s, cy_r, cz_s, cz_r, cc_s, cc_r, out_s, out_r, entered,
):
    dp, mp = lax.axis_index("dp"), lax.axis_index("mp")
    right, left, opposite = (mp + 1) % n_mp, (mp + n_mp - 1) % n_mp, (mp + 2) % n_mp
    core, y, z = dp % CORES, (dp // CORES) % Y, dp // (CORES * Y)

    def on_y(step):
        return (z * Y + (y + step) % Y) * CORES + core

    partner = dp + 1 - 2 * core

    def remote(src, dst, sends, receives, where):
        return pltpu.make_async_remote_copy(
            src_ref=src, dst_ref=dst, send_sem=sends, recv_sem=receives, device_id=where,
            device_id_type=pl.DeviceIdType.MESH,
        )

    draining = []

    def arrival(ref, receives):
        if draining:
            return
        remote(ref, ref, receives, receives, (dp, right)).wait_recv()

    def send(ref, sends, receives, where):
        copy = remote(ref, ref, sends, receives, where)
        if draining:
            copy.wait_send()
        else:
            copy.start()

    barrier = pltpu.get_barrier_semaphore()

    def greet(where):
        pl.semaphore_signal(barrier, inc=1, device_id=where, device_id_type=pl.DeviceIdType.MESH)

    def far_first(act):
        act(dp, n_dp // 2)

        def both(step, carry):
            act(dp, n_dp // 2 - step)
            act(dp, n_dp // 2 + step)
            return carry

        lax.fori_loop(1, n_dp // 2, both, 0)

    loads = [
        (selection_h, selection), (destination_h, destination), (pixels, pixels_v), (captions, captions_v),
        (position, place.at[mp]), (output_weight, wo.at[mp]), (patch_weight, patch_v), (gains_h, gains),
        (query_key_value, qkv_v), (loss_params_h, loss_params), (up_weight, up_v), (down_weight, down_v),
        (embedding_weight, embedding_v),
    ]
    loads = [pltpu.make_async_copy(a, b, local.at[n]) for n, (a, b) in enumerate(loads)]
    for load in loads[:4]:
        load.start()
    near = [(dp, opposite), (on_y(2), mp), (dp, right), (dp, left), (on_y(1), mp), (on_y(Y - 1), mp), (partner, mp)]
    n_z = n_dp // (Y * CORES)
    z_near = [((dp + step * Y * CORES) % n_dp, mp) for step in (1, n_z - 1)] if n_z > 1 else []
    for where in near + z_near:
        greet(where)
    for load in loads[4:]:
        load.start()

    loads[0].wait()
    loads[1].wait()
    index = [jnp.int32(0)] * SEND_MOST
    target = [jnp.int32(-1)] * SEND_MOST
    count = jnp.int32(0)
    for example in range(selection.shape[0]):
        chosen = selection[example] > 0
        goal = destination[example]
        for k in range(SEND_MOST):
            hit = jnp.logical_and(chosen, count == k)
            index[k] = jnp.where(hit, example, index[k])
            target[k] = jnp.where(hit, goal, target[k])
        count = count + chosen.astype(jnp.int32)

    loads[2].wait()
    for k in range(SEND_MOST):
        pix[k, mp] = pixels_v[index[k]]
    loads[3].wait()
    line = lax.broadcasted_iota(jnp.int32, (32, 16), 0) // 8
    wanted = jnp.where(line == 0, index[0], jnp.where(line == 1, index[1], index[2]))
    chosen_rows = (lax.broadcasted_iota(jnp.int32, (32, 16), 1) == wanted).astype(F32).astype(BF16)
    tiles = diagonal(dot(chosen_rows, captions_v[...]))
    for k in range(SEND_MOST):
        cap_send[k] = tiles[8 * k : 8 * k + 8].astype(BF16)
    lane = lax.broadcasted_iota(jnp.int32, (8, 128), 1)
    goals = jnp.where(lane == 0, target[0], jnp.where(lane == 1, target[1], jnp.where(lane == 2, target[2], -1)))
    cap_send[3] = goals.astype(F32).astype(BF16)
    caps[core, z, y] = cap_send[...]
    loads[4].wait()
    loads[5].wait()

    pl.semaphore_wait(barrier, len(near + z_near))

    def tell(step):
        for where in z_near if step else [(on_y(n), mp) for n in range(1, Y)]:
            pl.semaphore_signal(entered.at[step], inc=1, device_id=where, device_id_type=pl.DeviceIdType.MESH)

    def told(step):
        pl.semaphore_wait(entered.at[step], len(z_near) if step else Y - 1)

    tell(0)

    mp_peers = ((right, 0), (left, 1), (opposite, 2))
    mp_sources = ((left, 0), (right, 1), (opposite, 2))

    def halves(piece):
        half = piece.shape[0] // 2
        return piece.at[pl.ds(0, half)], piece.at[pl.ds(half, half)]

    def ring_send(piece, sends, receives, to_right, to_left):
        first, second = halves(piece)
        send(first, sends.at[0], receives.at[0], to_right)
        send(second, sends.at[2], receives.at[2], to_left)
        send(second, sends.at[1], receives.at[1], to_right)
        send(first, sends.at[3], receives.at[3], to_left)

    def ring_forward(from_left, from_right, sends, receives, to_right, to_left):
        first, second = halves(from_left)[0], halves(from_right)[1]
        arrival(first, receives.at[0])
        send(first, sends.at[4], receives.at[4], to_right)
        arrival(second, receives.at[2])
        send(second, sends.at[5], receives.at[5], to_left)

    def ring_near(from_left, from_right, receives):
        arrival(halves(from_left)[1], receives.at[1])
        arrival(halves(from_right)[0], receives.at[3])

    def ring_finish(from_left, from_right, far, receives):
        ring_near(from_left, from_right, receives)
        ring_far(far, receives)

    def ring_far(far, receives):
        arrival(halves(far)[0], receives.at[4])
        arrival(halves(far)[1], receives.at[5])

    to_right, to_left = (dp, right), (dp, left)
    patch_rows = pix.shape[2]
    rows = n_mp * patch_rows

    def pix_send(k):
        ring_send(pix.at[k, mp], pix_s.at[k], pix_r.at[k], to_right, to_left)

    def pix_forward(k):
        ring_forward(
            pix.at[k, left], pix.at[k, right], pix_s.at[k], pix_r.at[k], to_right, to_left
        )

    def place_x():
        for other, n in mp_peers:
            send(place.at[mp, core, y], px_s.at[n], px_r.at[n], (dp, other))

    def place_y():
        for source, n in mp_sources:
            arrival(place.at[source, core, y], px_r.at[n])
            for step in range(1, Y):
                send(
                    place.at[source, core, y], py_s.at[n, step - 1], py_r.at[n, step - 1], (on_y(step), mp)
                )

    def place_core():
        for source, n in mp_sources:
            for step in range(1, Y):
                arrival(place.at[source, core, (y + Y - step) % Y], py_r.at[n, step - 1])
            send(place.at[source, core], pc_s.at[n], pc_r.at[n], (partner, mp))

    def wo_x():
        ring_send(wo.at[mp, core, y], wx_s, wx_r, to_right, to_left)

    def wo_x_forward():
        ring_forward(wo.at[left, core, y], wo.at[right, core, y], wx_s, wx_r, to_right, to_left)

    def wo_y():
        ring_finish(wo.at[left, core, y], wo.at[right, core, y], wo.at[opposite, core, y], wx_r)
        for source, n in mp_sources:
            for step in (2, 1, 3):
                send(wo.at[source, core, y], wy_s.at[n, step - 1], wy_r.at[n, step - 1], (on_y(step), mp))

    def wo_core():
        for source, n in mp_sources:
            for step in range(1, Y):
                arrival(wo.at[source, core, (y + Y - step) % Y], wy_r.at[n, step - 1])
            send(wo.at[source, core], wc_s.at[n], wc_r.at[n], (partner, mp))

    def caps_y():
        for step in range(1, Y):
            send(caps.at[core, z, y], cy_s.at[step - 1], cy_r.at[step - 1], (on_y(step), mp))

    def caps_z():
        for step in range(1, Y):
            arrival(caps.at[core, z, (y + Y - step) % Y], cy_r.at[step - 1])
        for step in range(1, n_z):
            there = ((((z + step) % n_z) * Y + y) * CORES + core, mp)
            send(caps.at[core, z], cz_s.at[step - 1], cz_r.at[step - 1], there)

    def caps_core():
        for step in range(1, n_z):
            arrival(caps.at[core, (z + n_z - step) % n_z], cz_r.at[step - 1])
        send(caps.at[core], cc_s, cc_r, (partner, mp))

    place_x()
    pix_send(0)
    wo_x()
    caps_y()
    place_y()
    pix_send(1)
    told(0)
    tell(1)
    pix_forward(0)
    wo_x_forward()
    pix_send(2)
    told(1)
    tell(2)
    place_core()
    told(2)
    tell(3)
    pix_forward(1)
    loads[6].wait()
    loads[7].wait()
    loads[8].wait()

    gain0, gain1 = gains[0:1, :], gains[1:2, :]
    width = gains.shape[1]
    chunk_rows = 32

    def norm_into(k, gain):
        def one(part, carry):
            span = pl.ds(pl.multiple_of(part * chunk_rows, chunk_rows), chunk_rows)
            normed[span, :] = norm_rows(hid[k, span, :], gain).astype(BF16)
            return carry

        lax.fori_loop(0, rows // chunk_rows, one, 0, unroll=4)

    half_lane = lax.broadcasted_iota(jnp.int32, (rows, 128), 1) < HEAD_DIM
    ones = jnp.ones((rows, 128), BF16)

    def ctx_send(k):
        ring_send(ctx.at[k, mp], ctx_s.at[k], ctx_r.at[k], to_right, to_left)

    def ctx_forward(k):
        ring_forward(ctx.at[k, left], ctx.at[k, right], ctx_s.at[k], ctx_r.at[k], to_right, to_left)

    def attend(k, carry):
        ring_finish(pix.at[k, left], pix.at[k, right], pix.at[k, opposite], pix_r.at[k])
        image = pix[k].reshape(rows, pix.shape[3])
        hid[k] = dot(image, patch_v[...])

        @pl.when(k == 0)
        def _():
            for source, n in mp_sources:
                arrival(place.at[source, 1 - core], pc_r.at[n])
            told(3)
            tell(4)
            wo_y()

        hid[k] = hid[k] + place[...].astype(F32).reshape(rows, width)
        norm_into(k, gain0)
        qkv[0] = (dot(normed[...], qkv_v[0]).astype(BF16) * BF16(HEAD_DIM ** (-0.5))).astype(BF16)
        qkv[1] = dot(normed[...], qkv_v[1]).astype(BF16)
        qkv[2] = dot(normed[...], qkv_v[2]).astype(BF16)
        @pl.when(k == 0)
        def _():
            pix_forward(2)

        for pair in range(qkv.shape[2] // 128):
            span = slice(pair * 128, pair * 128 + 128)
            query, keys, values = qkv[0, :, span], qkv[1, :, span], qkv[2, :, span]
            widened = jnp.concatenate([values, ones], axis=1)
            outs = []
            for head in range(2):
                mask = half_lane if head == 0 else jnp.logical_not(half_lane)
                mine = jnp.where(mask, query, jnp.zeros_like(query))
                scores = lax.dot_general(mine, keys, NT, preferred_element_type=F32)
                raised = jnp.exp(scores - jnp.max(scores, axis=1, keepdims=True)).astype(BF16)
                both = dot(raised, widened)
                outs.append(both[:, :128] / both[:, 128:])
            ctx[k, mp, :, span] = jnp.where(half_lane, outs[0], outs[1]).astype(BF16)

        ctx_send(k)

        @pl.when(k == 0)
        def _():
            told(4)
            caps_z()

        @pl.when(k == 1)
        def _():
            ctx_forward(0)

        return carry

    lax.fori_loop(0, SEND_MOST, attend, 0)
    ctx_forward(1)
    wo_core()
    caps_core()

    for source, n in mp_sources:
        arrival(wo.at[source, 1 - core], wc_r.at[n])
    loads[10].wait()

    def expand(k, carry):
        ring_near(ctx.at[k, left], ctx.at[k, right], ctx_r.at[k])
        context = jnp.concatenate([ctx[k, source] for source in (mp, left, right)], axis=1)
        weights = jnp.concatenate([wo[source].reshape(-1, width) for source in (mp, left, right)], axis=0)
        hid[k] = hid[k] + dot(context, weights)
        ring_far(ctx.at[k, opposite], ctx_r.at[k])
        hid[k] = hid[k] + dot(ctx[k, opposite], wo[opposite].reshape(-1, width))
        norm_into(k, gain1)
        own = jnp.sum(hid[k, pl.ds(pl.multiple_of(mp * patch_rows, patch_rows), patch_rows), :], axis=0, keepdims=True)
        shared[mp, k] = diagonal(jnp.broadcast_to(own, (8, width)))
        block = 512
        for n in range(up_v.shape[1] // block):
            span = slice(n * block, n * block + block)
            units = jax.nn.gelu(dot(normed[...], up_v[:, span]))
            total = jnp.sum(units, axis=0, keepdims=True)
            summed[k, :, span] = jnp.broadcast_to(total, (8, block))

        @pl.when(k == 0)
        def _():
            ctx_forward(2)

        return carry

    lax.fori_loop(0, SEND_MOST, expand, 0)

    loads[11].wait()
    totals = summed[...].reshape(SEND_MOST * 8, width)
    high = totals.astype(BF16)
    low = (totals - high.astype(F32)).astype(BF16)
    down = dot(jnp.concatenate([high, low], axis=0), down_v[...])
    down = down[: SEND_MOST * 8] + down[SEND_MOST * 8 :]
    shared[mp] = shared[mp] + diagonal(down).reshape(SEND_MOST, 8, 128)

    def share():
        for other, n in mp_peers:
            send(shared.at[mp], ar_s.at[n], ar_r.at[n], (dp, other))

    share()
    arrival(caps.at[1 - core], cc_r)
    caps_all = caps[...].reshape(n_dp, SEND_MOST + 1, 8, 128)
    flat = n_dp * 8
    goals = caps_all[:, 3].astype(F32).reshape(flat, 128)
    here = goals == dp.astype(F32)
    match = jnp.where(here, 1.0, 0.0)
    present = jnp.broadcast_to(jnp.sum(match, axis=1, keepdims=True), (flat, 128))
    row, column = (lax.broadcasted_iota(jnp.int32, (flat, flat), n) for n in range(2))
    row_dp, column_dp = (n // 8 % (n_dp // CORES) * CORES + n // 8 // (n_dp // CORES) for n in (row, column))
    earlier = jnp.where(jnp.logical_and(row_dp > column_dp, column % 8 == 0), 1.0, 0.0).astype(BF16)
    order = dot(earlier, present.astype(BF16))
    lane = lax.broadcasted_iota(jnp.int32, (flat, 128), 1)
    line = lax.broadcasted_iota(jnp.int32, (flat, 128), 0)
    in_slot = jnp.where(order == (lane % 4).astype(F32), present, 0.0)
    spread = jnp.where(jnp.logical_and(line % 8 == lane // 16, lane % 16 < 12), in_slot, 0.0)
    picker[...] = spread.T.astype(BF16)
    filled = jnp.sum(jnp.max(in_slot.reshape(n_dp, 8, 128), axis=1), axis=0, keepdims=True)
    loads[9].wait()
    scale = 10.0 * jnp.exp(jnp.full((1, 128), loss_params[0], F32))
    shift = 2.0 * jnp.full((1, 128), loss_params[1], F32)
    for k in range(SEND_MOST):
        tiles = caps_all[:, k].astype(F32)
        caps_flat[pl.ds(k * flat, flat), :] = tiles.reshape(flat, 128).astype(BF16)
        square = jnp.sum(jnp.sum(tiles * tiles, axis=1), axis=1, keepdims=True)
        length = lax.rsqrt(square / width + EPS) * width ** (-0.5)
        weight_of[k] = length * scale
        column_of = jnp.sum(jnp.where(lane == k, match, 0.0), axis=1, keepdims=True)
        same = jnp.max((column_of * in_slot).reshape(n_dp, 8, 128), axis=1)
        alive = jnp.max(jnp.where(lane == k, goals, -1.0), axis=1, keepdims=True)
        alive = jnp.max(jnp.broadcast_to(alive, (flat, 128)).reshape(n_dp, 8, 128), axis=1)
        sign_of[k] = jnp.where(alive >= 0.0, 1.0 - 2.0 * same, 0.0)
    for source, n in mp_sources:
        arrival(shared.at[source], ar_r.at[n])
    pooled = (shared[0] + shared[1]) + (shared[2] + shared[3])
    pooled = pooled / rows

    def mean_of(tiles):
        return jnp.sum(jnp.sum(tiles, axis=2, keepdims=True), axis=1, keepdims=True) / width

    centred = pooled - mean_of(pooled)
    gain2 = diagonal(jnp.broadcast_to(gains[2:3, :], (8, width)))
    ready = centred * lax.rsqrt(mean_of(centred * centred) + EPS) * gain2[None]
    goal_of = lax.broadcasted_iota(jnp.int32, (n_dp, 8, 128), 0)
    outgoing = jnp.zeros((n_dp, 8, 128), F32)
    for k in range(SEND_MOST):
        outgoing = jnp.where(goal_of == target[k], ready[k][None], outgoing)
    out_send[...] = outgoing.astype(BF16)
    spot = core * (n_dp // CORES) + dp // CORES
    arrived[spot] = out_send[dp]

    def deliver(me, step):
        there = (me + step) % n_dp
        remote(out_send.at[there], arrived.at[spot], out_s, out_r, (there, mp)).start()

    far_first(deliver)
    loads[12].wait()
    others = arrived.at[pl.ds(0, n_dp - 1)]
    pltpu.make_async_copy(others, others, out_r).wait()

    slots = dot(picker[...], arrived[...].astype(F32).reshape(flat, 128).astype(BF16)).astype(BF16)
    slots = jnp.concatenate([slots[n * 16 : n * 16 + 16] for n in range(8)], axis=1)
    embedded = dot(slots, embedding_v[...])
    embedded_out[...] = embedded[:RECV_MOST]
    unit = embedded * (lax.rsqrt(jnp.mean(embedded * embedded, axis=1, keepdims=True) + EPS) * width ** (-0.5))
    first = unit.astype(BF16).astype(F32)
    rest = unit - first
    second = rest.astype(BF16).astype(F32)
    line = lax.broadcasted_iota(jnp.int32, unit.shape, 0)
    parts = jnp.where(line < 4, first, jnp.where(line < 8, second, jnp.where(line < 12, rest - second, 0.0)))
    parts = parts.astype(BF16)
    parts = jnp.concatenate([parts[:, n * 128 : n * 128 + 128] for n in range(8)], axis=0)
    products = lax.dot_general(caps_flat[...], parts, NT, preferred_element_type=F32)
    line = lax.broadcasted_iota(jnp.int32, (SEND_MOST * flat, 128), 0)
    lane = lax.broadcasted_iota(jnp.int32, (SEND_MOST * flat, 128), 1)
    products = jnp.where(line % 8 == lane // 16, products, 0.0).reshape(SEND_MOST * n_dp, 8, 128)
    products = jnp.sum(products, axis=1)
    for step in (64, 32, 16, 8, 4):
        products = products + pltpu.roll(products, step, 1)
    weights = weight_of[...].reshape(SEND_MOST * n_dp, 128)
    signs = sign_of[...].reshape(SEND_MOST * n_dp, 128)
    terms = signs * (products * weights + shift)
    terms = jnp.maximum(terms, 0.0) + jnp.log1p(jnp.exp(-jnp.abs(terms)))
    terms = jnp.where(signs == 0.0, 0.0, terms)
    losses = jnp.sum(terms, axis=0, keepdims=True) / float(n_dp * SEL_DEV)
    losses_out[...] = jnp.where(filled > 0.0, losses, 0.0)

    draining.append(True)
    for act in (place_x, place_y, place_core, wo_x, wo_x_forward, wo_y, wo_core, caps_y, caps_z, caps_core, share):
        act()
    for k in range(SEND_MOST):
        for act in (pix_send, pix_forward, ctx_send, ctx_forward):
            act(k)
    others = arrived.at[pl.ds(0, n_dp - 1)]
    pltpu.make_async_copy(others, others, out_s).wait()


def hand_over(embedded, losses, embedded_out, losses_out):
    embedded_out[...] = embedded[...]
    losses_out[...] = losses[0, :RECV_MOST]


def per_device(
    pixels, selection, destination, patch_weight, position, query_key_value, output_weight, up_weight,
    down_weight, norm_gains, embedding_weight, caption_vectors, loss_params,
):
    n_dp, n_mp = lax.axis_size("dp"), lax.axis_size("mp")
    width, units = up_weight.shape
    share = query_key_value.shape[2]
    patch_rows, values = pixels.shape[1:]
    rows = n_mp * patch_rows
    place_rows = position.shape[0] // (Y * CORES)
    slice_rows = output_weight.shape[0] // (Y * CORES)
    position = position.reshape(CORES, Y, place_rows, width)
    output_weight = output_weight.reshape(CORES, Y, slice_rows, width)
    vmem = pl.BlockSpec(memory_space=pltpu.VMEM)
    far = pl.BlockSpec(memory_space=pl.ANY)
    dma = pltpu.SemaphoreType.DMA
    n = SEND_MOST
    scratch = [
        pltpu.SMEM(selection.shape, jnp.int32), pltpu.SMEM(destination.shape, jnp.int32),
        pltpu.SMEM(loss_params.shape, F32), pltpu.VMEM(norm_gains.shape, F32),
        pltpu.VMEM(pixels.shape, BF16), pltpu.VMEM(patch_weight.shape, BF16),
        pltpu.VMEM(query_key_value.shape, BF16), pltpu.VMEM(up_weight.shape, BF16),
        pltpu.VMEM(down_weight.shape, BF16), pltpu.VMEM(embedding_weight.shape, BF16),
        pltpu.VMEM(caption_vectors.shape, BF16),
        pltpu.VMEM((n, n_mp, patch_rows, values), BF16),
        pltpu.VMEM((n_mp, CORES, Y, place_rows, width), BF16),
        pltpu.VMEM((n_mp, CORES, Y, slice_rows, width), BF16),
        pltpu.VMEM((n, rows, width), F32), pltpu.VMEM((rows, width), BF16),
        pltpu.VMEM((3, rows, share), BF16), pltpu.VMEM((n, n_mp, rows, share), BF16),
        pltpu.VMEM((n + 1, 8, 128), BF16), pltpu.VMEM((CORES, n_dp // (CORES * Y), Y, n + 1, 8, 128), BF16),
        pltpu.VMEM((n * n_dp * 8, 128), BF16), pltpu.VMEM((n, 8, units), F32),
        pltpu.VMEM((n_mp, n, 8, 128), F32),
        pltpu.VMEM((n_dp, 8, 128), BF16), pltpu.VMEM((n_dp, 8, 128), BF16),
        pltpu.VMEM((128, n_dp * 8), BF16), pltpu.VMEM((n, n_dp, 128), F32), pltpu.VMEM((n, n_dp, 128), F32),
        dma((13,)), dma((n, 6)), dma((n, 6)), dma((3,)), dma((3,)), dma((3, 3)), dma((3, 3)), dma((3,)), dma((3,)),
        dma((6,)), dma((6,)), dma((3, 3)), dma((3, 3)), dma((3,)), dma((3,)),
        dma((n, 6)), dma((n, 6)), dma((3,)), dma((3,)), dma((3,)), dma((3,)),
        dma((7,)), dma((7,)), dma, dma, dma, dma, pltpu.SemaphoreType.REGULAR((5,)),
    ]
    embedded, losses = pl.pallas_call(
        functools.partial(body, n_dp, n_mp),
        out_shape=(
            jax.ShapeDtypeStruct((RECV_MOST, width), F32),
            jax.ShapeDtypeStruct((1, 128), F32),
        ),
        in_specs=[far] * 13,
        out_specs=(vmem, vmem),
        scratch_shapes=scratch,
        name="learner",
        compiler_params=pltpu.CompilerParams(
            collective_id=0, has_side_effects=True, vmem_limit_bytes=60 * 1024 * 1024
        ),
    )(
        selection, destination, loss_params, pixels, patch_weight, position, query_key_value, output_weight,
        up_weight, down_weight, norm_gains, embedding_weight, caption_vectors,
    )
    return pl.pallas_call(
        hand_over,
        out_shape=(jax.ShapeDtypeStruct((RECV_MOST, width), F32), jax.ShapeDtypeStruct((RECV_MOST,), F32)),
        name="hand_over",
    )(embedded, losses)


def solution(mesh):
    in_specs = (
        P("dp", "mp", None), P("dp"), P("dp"), P(), P("mp", None), P(None, None, "mp"), P("mp", None),
        P(None, "mp"), P("mp", None), P(), P(), P("dp", None), P(),
    )
    out_specs = (P("dp", None), P("dp"))
    return jax.shard_map(per_device, mesh=mesh, in_specs=in_specs, out_specs=out_specs, check_vma=False)
```

```python
import functools

import jax
import jax.numpy as jnp
from jax import lax
from jax.experimental import pallas as pl
from jax.experimental.pallas import tpu as pltpu
from jax.sharding import PartitionSpec as P

EPS = 1e-06
SEND_MOST = 3
RECV_MOST = 4
SEL_DEV = 2
HEAD_DIM = 64
Y, CORES = 4, 2
F32, BF16 = jnp.float32, jnp.bfloat16
NT = (((1,), (1,)), ((), ()))


def norm_rows(values, gain):
    center = jnp.mean(values, axis=-1, keepdims=True)
    centred = values - center
    spread = jnp.mean(centred * centred, axis=-1, keepdims=True)
    return centred * lax.rsqrt(spread + EPS) * gain


def diagonal(rows):
    count = rows.shape[0]
    line = lax.broadcasted_iota(jnp.int32, (count, 128), 0) % 8
    out = jnp.zeros((count, 128), rows.dtype)
    for chunk in range(8):
        out = jnp.where(line == chunk, rows[:, chunk * 128 : (chunk + 1) * 128], out)
    return out


def dot(a, b):
    return jnp.dot(a, b, preferred_element_type=F32)


def body(
    n_dp, n_mp,
    selection_h, destination_h, loss_params_h, pixels, patch_weight, position, query_key_value, output_weight,
    up_weight, down_weight, gains_h, embedding_weight, captions,
    embedded_out, losses_out,
    selection, destination, loss_params, gains, pixels_v, patch_v, qkv_v, up_v, down_v, embedding_v, captions_v,
    pix, place, wo, hid, normed, qkv, ctx, cap_send, caps, caps_flat, summed, shared,
    out_send, arrived, picker, sign_of, weight_of,
    local, pix_s, pix_r, px_s, px_r, py_s, py_r, pc_s, pc_r, wx_s, wx_r, wy_s, wy_r, wc_s, wc_r,
    ctx_s, ctx_r, ar_s, ar_r, cy_s, cy_r, cz_s, cz_r, cc_s, cc_r, out_s, out_r, entered,
):
    dp, mp = lax.axis_index("dp"), lax.axis_index("mp")
    right, left, opposite = (mp + 1) % n_mp, (mp + n_mp - 1) % n_mp, (mp + 2) % n_mp
    core, y, z = dp % CORES, (dp // CORES) % Y, dp // (CORES * Y)

    def on_y(step):
        return (z * Y + (y + step) % Y) * CORES + core

    partner = dp + 1 - 2 * core

    def remote(src, dst, sends, receives, where):
        return pltpu.make_async_remote_copy(
            src_ref=src, dst_ref=dst, send_sem=sends, recv_sem=receives, device_id=where,
            device_id_type=pl.DeviceIdType.MESH,
        )

    draining = []

    def arrival(ref, receives):
        if draining:
            return
        remote(ref, ref, receives, receives, (dp, right)).wait_recv()

    def send(ref, sends, receives, where):
        copy = remote(ref, ref, sends, receives, where)
        if draining:
            copy.wait_send()
        else:
            copy.start()

    barrier = pltpu.get_barrier_semaphore()

    def greet(where):
        pl.semaphore_signal(barrier, inc=1, device_id=where, device_id_type=pl.DeviceIdType.MESH)

    def far_first(act):
        act(dp, n_dp // 2)

        def both(step, carry):
            act(dp, n_dp // 2 - step)
            act(dp, n_dp // 2 + step)
            return carry

        lax.fori_loop(1, n_dp // 2, both, 0, unroll=True)

    loads = [
        (selection_h, selection), (destination_h, destination), (pixels, pixels_v), (captions, captions_v),
        (position, place.at[mp]), (output_weight, wo.at[mp]), (patch_weight, patch_v), (gains_h, gains),
        (query_key_value, qkv_v), (loss_params_h, loss_params), (up_weight, up_v), (down_weight, down_v),
        (embedding_weight, embedding_v),
    ]
    loads = [pltpu.make_async_copy(a, b, local.at[n]) for n, (a, b) in enumerate(loads)]
    for load in loads[:4]:
        load.start()
    near = [(dp, opposite), (on_y(2), mp), (dp, right), (dp, left), (on_y(1), mp), (on_y(Y - 1), mp), (partner, mp)]
    n_z = n_dp // (Y * CORES)
    z_near = [((dp + step * Y * CORES) % n_dp, mp) for step in (1, n_z - 1)] if n_z > 1 else []
    for where in near + z_near:
        greet(where)
    for load in loads[4:]:
        load.start()

    loads[0].wait()
    loads[1].wait()
    index = [jnp.int32(0)] * SEND_MOST
    target = [jnp.int32(-1)] * SEND_MOST
    count = jnp.int32(0)
    for example in range(selection.shape[0]):
        chosen = selection[example] > 0
        goal = destination[example]
        for k in range(SEND_MOST):
            hit = jnp.logical_and(chosen, count == k)
            index[k] = jnp.where(hit, example, index[k])
            target[k] = jnp.where(hit, goal, target[k])
        count = count + chosen.astype(jnp.int32)

    loads[2].wait()
    for k in range(SEND_MOST):
        pix[k, mp] = pixels_v[index[k]]
    loads[3].wait()
    line = lax.broadcasted_iota(jnp.int32, (32, 16), 0) // 8
    wanted = jnp.where(line == 0, index[0], jnp.where(line == 1, index[1], index[2]))
    chosen_rows = (lax.broadcasted_iota(jnp.int32, (32, 16), 1) == wanted).astype(F32).astype(BF16)
    tiles = diagonal(dot(chosen_rows, captions_v[...]))
    for k in range(SEND_MOST):
        cap_send[k] = tiles[8 * k : 8 * k + 8].astype(BF16)
    lane = lax.broadcasted_iota(jnp.int32, (8, 128), 1)
    goals = jnp.where(lane == 0, target[0], jnp.where(lane == 1, target[1], jnp.where(lane == 2, target[2], -1)))
    cap_send[3] = goals.astype(F32).astype(BF16)
    caps[core, z, y] = cap_send[...]
    loads[4].wait()
    loads[5].wait()

    pl.semaphore_wait(barrier, len(near + z_near))

    def tell(step):
        for where in z_near if step else [(on_y(n), mp) for n in range(1, Y)]:
            pl.semaphore_signal(entered.at[step], inc=1, device_id=where, device_id_type=pl.DeviceIdType.MESH)

    def told(step):
        pl.semaphore_wait(entered.at[step], len(z_near) if step else Y - 1)

    tell(0)

    mp_peers = ((right, 0), (left, 1), (opposite, 2))
    mp_sources = ((left, 0), (right, 1), (opposite, 2))

    def halves(piece):
        half = piece.shape[0] // 2
        return piece.at[pl.ds(0, half)], piece.at[pl.ds(half, half)]

    def ring_send(piece, sends, receives, to_right, to_left):
        first, second = halves(piece)
        send(first, sends.at[0], receives.at[0], to_right)
        send(second, sends.at[2], receives.at[2], to_left)
        send(second, sends.at[1], receives.at[1], to_right)
        send(first, sends.at[3], receives.at[3], to_left)

    def ring_forward(from_left, from_right, sends, receives, to_right, to_left):
        first, second = halves(from_left)[0], halves(from_right)[1]
        arrival(first, receives.at[0])
        send(first, sends.at[4], receives.at[4], to_right)
        arrival(second, receives.at[2])
        send(second, sends.at[5], receives.at[5], to_left)

    def ring_near(from_left, from_right, receives):
        arrival(halves(from_left)[1], receives.at[1])
        arrival(halves(from_right)[0], receives.at[3])

    def ring_finish(from_left, from_right, far, receives):
        ring_near(from_left, from_right, receives)
        ring_far(far, receives)

    def ring_far(far, receives):
        arrival(halves(far)[0], receives.at[4])
        arrival(halves(far)[1], receives.at[5])

    to_right, to_left = (dp, right), (dp, left)
    patch_rows = pix.shape[2]
    rows = n_mp * patch_rows

    def pix_send(k):
        ring_send(pix.at[k, mp], pix_s.at[k], pix_r.at[k], to_right, to_left)

    def pix_forward(k):
        ring_forward(
            pix.at[k, left], pix.at[k, right], pix_s.at[k], pix_r.at[k], to_right, to_left
        )

    def place_x():
        for other, n in mp_peers:
            send(place.at[mp, core, y], px_s.at[n], px_r.at[n], (dp, other))

    def place_y():
        for source, n in mp_sources:
            arrival(place.at[source, core, y], px_r.at[n])
            for step in range(1, Y):
                send(
                    place.at[source, core, y], py_s.at[n, step - 1], py_r.at[n, step - 1], (on_y(step), mp)
                )

    def place_core():
        for source, n in mp_sources:
            for step in range(1, Y):
                arrival(place.at[source, core, (y + Y - step) % Y], py_r.at[n, step - 1])
            send(place.at[source, core], pc_s.at[n], pc_r.at[n], (partner, mp))

    def wo_x():
        ring_send(wo.at[mp, core, y], wx_s, wx_r, to_right, to_left)

    def wo_x_forward():
        ring_forward(wo.at[left, core, y], wo.at[right, core, y], wx_s, wx_r, to_right, to_left)

    def wo_y():
        ring_finish(wo.at[left, core, y], wo.at[right, core, y], wo.at[opposite, core, y], wx_r)
        for source, n in mp_sources:
            for step in (2, 1, 3):
                send(wo.at[source, core, y], wy_s.at[n, step - 1], wy_r.at[n, step - 1], (on_y(step), mp))

    def wo_core():
        for source, n in mp_sources:
            for step in range(1, Y):
                arrival(wo.at[source, core, (y + Y - step) % Y], wy_r.at[n, step - 1])
            send(wo.at[source, core], wc_s.at[n], wc_r.at[n], (partner, mp))

    def caps_y():
        for step in range(1, Y):
            send(caps.at[core, z, y], cy_s.at[step - 1], cy_r.at[step - 1], (on_y(step), mp))

    def caps_z():
        for step in range(1, Y):
            arrival(caps.at[core, z, (y + Y - step) % Y], cy_r.at[step - 1])
        for step in range(1, n_z):
            there = ((((z + step) % n_z) * Y + y) * CORES + core, mp)
            send(caps.at[core, z], cz_s.at[step - 1], cz_r.at[step - 1], there)

    def caps_core():
        for step in range(1, n_z):
            arrival(caps.at[core, (z + n_z - step) % n_z], cz_r.at[step - 1])
        send(caps.at[core], cc_s, cc_r, (partner, mp))

    place_x()
    pix_send(0)
    wo_x()
    caps_y()
    place_y()
    pix_send(1)
    told(0)
    tell(1)
    pix_forward(0)
    wo_x_forward()
    told(1)
    tell(2)
    place_core()
    told(2)
    tell(3)
    pix_forward(1)
    pix_send(2)
    loads[6].wait()
    loads[7].wait()
    loads[8].wait()

    gain0, gain1 = gains[0:1, :], gains[1:2, :]
    width = gains.shape[1]
    chunk_rows = 32

    def norm_into(k, gain):
        def one(part, carry):
            span = pl.ds(pl.multiple_of(part * chunk_rows, chunk_rows), chunk_rows)
            normed[span, :] = norm_rows(hid[k, span, :], gain).astype(BF16)
            return carry

        lax.fori_loop(0, rows // chunk_rows, one, 0, unroll=4)

    half_lane = lax.broadcasted_iota(jnp.int32, (rows, 128), 1) < HEAD_DIM
    ones = jnp.ones((rows, 128), BF16)

    def ctx_send(k):
        ring_send(ctx.at[k, mp], ctx_s.at[k], ctx_r.at[k], to_right, to_left)

    def ctx_forward(k):
        ring_forward(ctx.at[k, left], ctx.at[k, right], ctx_s.at[k], ctx_r.at[k], to_right, to_left)

    def attend(k, carry):
        ring_finish(pix.at[k, left], pix.at[k, right], pix.at[k, opposite], pix_r.at[k])
        image = pix[k].reshape(rows, pix.shape[3])
        hid[k] = dot(image, patch_v[...])

        @pl.when(k == 0)
        def _():
            for source, n in mp_sources:
                arrival(place.at[source, 1 - core], pc_r.at[n])
            told(3)
            tell(4)
            wo_y()

        hid[k] = hid[k] + place[...].astype(F32).reshape(rows, width)
        norm_into(k, gain0)
        qkv[0] = (dot(normed[...], qkv_v[0]).astype(BF16) * BF16(HEAD_DIM ** (-0.5))).astype(BF16)
        qkv[1] = dot(normed[...], qkv_v[1]).astype(BF16)
        qkv[2] = dot(normed[...], qkv_v[2]).astype(BF16)
        @pl.when(k == 0)
        def _():
            pix_forward(2)

        for pair in range(qkv.shape[2] // 128):
            span = slice(pair * 128, pair * 128 + 128)
            query, keys, values = qkv[0, :, span], qkv[1, :, span], qkv[2, :, span]
            widened = jnp.concatenate([values, ones], axis=1)
            outs = []
            for head in range(2):
                mask = half_lane if head == 0 else jnp.logical_not(half_lane)
                mine = jnp.where(mask, query, jnp.zeros_like(query))
                scores = lax.dot_general(mine, keys, NT, preferred_element_type=F32)
                raised = jnp.exp(scores - jnp.max(scores, axis=1, keepdims=True)).astype(BF16)
                both = dot(raised, widened)
                outs.append(both[:, :128] / both[:, 128:])
            ctx[k, mp, :, span] = jnp.where(half_lane, outs[0], outs[1]).astype(BF16)

        ctx_send(k)

        @pl.when(k == 0)
        def _():
            told(4)
            caps_z()

        @pl.when(k == 1)
        def _():
            ctx_forward(0)

        return carry

    lax.fori_loop(0, SEND_MOST, attend, 0)
    ctx_forward(1)
    wo_core()
    caps_core()

    for source, n in mp_sources:
        arrival(wo.at[source, 1 - core], wc_r.at[n])
    loads[10].wait()

    def expand(k, carry):
        ring_near(ctx.at[k, left], ctx.at[k, right], ctx_r.at[k])
        context = jnp.concatenate([ctx[k, source] for source in (mp, left, right)], axis=1)
        weights = jnp.concatenate([wo[source].reshape(-1, width) for source in (mp, left, right)], axis=0)
        hid[k] = hid[k] + dot(context, weights)
        ring_far(ctx.at[k, opposite], ctx_r.at[k])
        hid[k] = hid[k] + dot(ctx[k, opposite], wo[opposite].reshape(-1, width))
        norm_into(k, gain1)
        own = jnp.sum(hid[k, pl.ds(pl.multiple_of(mp * patch_rows, patch_rows), patch_rows), :], axis=0, keepdims=True)
        shared[mp, k] = diagonal(jnp.broadcast_to(own, (8, width)))
        block = 512
        for n in range(up_v.shape[1] // block):
            span = slice(n * block, n * block + block)
            units = jax.nn.gelu(dot(normed[...], up_v[:, span]))
            total = jnp.sum(units, axis=0, keepdims=True)
            summed[k, :, span] = jnp.broadcast_to(total, (8, block))

        @pl.when(k == 0)
        def _():
            ctx_forward(2)

        return carry

    lax.fori_loop(0, SEND_MOST, expand, 0)

    loads[11].wait()
    totals = summed[...].reshape(SEND_MOST * 8, width)
    high = totals.astype(BF16)
    low = (totals - high.astype(F32)).astype(BF16)
    down = dot(jnp.concatenate([high, low], axis=0), down_v[...])
    down = down[: SEND_MOST * 8] + down[SEND_MOST * 8 :]
    shared[mp] = shared[mp] + diagonal(down).reshape(SEND_MOST, 8, 128)

    def share():
        for other, n in mp_peers:
            send(shared.at[mp], ar_s.at[n], ar_r.at[n], (dp, other))

    share()
    arrival(caps.at[1 - core], cc_r)
    caps_all = caps[...].reshape(n_dp, SEND_MOST + 1, 8, 128)
    flat = n_dp * 8
    goals = caps_all[:, 3].astype(F32).reshape(flat, 128)
    here = goals == dp.astype(F32)
    match = jnp.where(here, 1.0, 0.0)
    present = jnp.broadcast_to(jnp.sum(match, axis=1, keepdims=True), (flat, 128))
    row, column = (lax.broadcasted_iota(jnp.int32, (flat, flat), n) for n in range(2))
    row_dp, column_dp = (n // 8 % (n_dp // CORES) * CORES + n // 8 // (n_dp // CORES) for n in (row, column))
    earlier = jnp.where(jnp.logical_and(row_dp > column_dp, column % 8 == 0), 1.0, 0.0).astype(BF16)
    order = dot(earlier, present.astype(BF16))
    lane = lax.broadcasted_iota(jnp.int32, (flat, 128), 1)
    line = lax.broadcasted_iota(jnp.int32, (flat, 128), 0)
    in_slot = jnp.where(order == (lane % 4).astype(F32), present, 0.0)
    spread = jnp.where(jnp.logical_and(line % 8 == lane // 16, lane % 16 < 12), in_slot, 0.0)
    picker[...] = spread.T.astype(BF16)
    filled = jnp.sum(jnp.max(in_slot.reshape(n_dp, 8, 128), axis=1), axis=0, keepdims=True)
    loads[9].wait()
    scale = 10.0 * jnp.exp(jnp.full((1, 128), loss_params[0], F32))
    shift = 2.0 * jnp.full((1, 128), loss_params[1], F32)
    for k in range(SEND_MOST):
        tiles = caps_all[:, k].astype(F32)
        caps_flat[pl.ds(k * flat, flat), :] = tiles.reshape(flat, 128).astype(BF16)
        square = jnp.sum(jnp.sum(tiles * tiles, axis=1), axis=1, keepdims=True)
        length = lax.rsqrt(square / width + EPS) * width ** (-0.5)
        weight_of[k] = length * scale
        column_of = jnp.sum(jnp.where(lane == k, match, 0.0), axis=1, keepdims=True)
        same = jnp.max((column_of * in_slot).reshape(n_dp, 8, 128), axis=1)
        alive = jnp.max(jnp.where(lane == k, goals, -1.0), axis=1, keepdims=True)
        alive = jnp.max(jnp.broadcast_to(alive, (flat, 128)).reshape(n_dp, 8, 128), axis=1)
        sign_of[k] = jnp.where(alive >= 0.0, 1.0 - 2.0 * same, 0.0)
    for source, n in mp_sources:
        arrival(shared.at[source], ar_r.at[n])
    pooled = (shared[0] + shared[1]) + (shared[2] + shared[3])
    pooled = pooled / rows

    def mean_of(tiles):
        return jnp.sum(jnp.sum(tiles, axis=2, keepdims=True), axis=1, keepdims=True) / width

    centred = pooled - mean_of(pooled)
    gain2 = diagonal(jnp.broadcast_to(gains[2:3, :], (8, width)))
    ready = centred * lax.rsqrt(mean_of(centred * centred) + EPS) * gain2[None]
    goal_of = lax.broadcasted_iota(jnp.int32, (n_dp, 8, 128), 0)
    outgoing = jnp.zeros((n_dp, 8, 128), F32)
    for k in range(SEND_MOST):
        outgoing = jnp.where(goal_of == target[k], ready[k][None], outgoing)
    out_send[...] = outgoing.astype(BF16)
    spot = core * (n_dp // CORES) + dp // CORES
    arrived[spot] = out_send[dp]

    def deliver(me, step):
        there = (me + step) % n_dp
        remote(out_send.at[there], arrived.at[spot], out_s, out_r, (there, mp)).start()

    far_first(deliver)
    loads[12].wait()
    others = arrived.at[pl.ds(0, n_dp - 1)]
    pltpu.make_async_copy(others, others, out_r).wait()

    slots = dot(picker[...], arrived[...].astype(F32).reshape(flat, 128).astype(BF16)).astype(BF16)
    slots = jnp.concatenate([slots[n * 16 : n * 16 + 16] for n in range(8)], axis=1)
    embedded = dot(slots, embedding_v[...])
    embedded_out[...] = embedded[:RECV_MOST]
    unit = embedded * (lax.rsqrt(jnp.mean(embedded * embedded, axis=1, keepdims=True) + EPS) * width ** (-0.5))
    first = unit.astype(BF16).astype(F32)
    rest = unit - first
    second = rest.astype(BF16).astype(F32)
    line = lax.broadcasted_iota(jnp.int32, unit.shape, 0)
    parts = jnp.where(line < 4, first, jnp.where(line < 8, second, jnp.where(line < 12, rest - second, 0.0)))
    parts = parts.astype(BF16)
    parts = jnp.concatenate([parts[:, n * 128 : n * 128 + 128] for n in range(8)], axis=0)
    products = lax.dot_general(caps_flat[...], parts, NT, preferred_element_type=F32)
    line = lax.broadcasted_iota(jnp.int32, (SEND_MOST * flat, 128), 0)
    lane = lax.broadcasted_iota(jnp.int32, (SEND_MOST * flat, 128), 1)
    products = jnp.where(line % 8 == lane // 16, products, 0.0).reshape(SEND_MOST * n_dp, 8, 128)
    products = jnp.sum(products, axis=1)
    for step in (64, 32, 16, 8, 4):
        products = products + pltpu.roll(products, step, 1)
    weights = weight_of[...].reshape(SEND_MOST * n_dp, 128)
    signs = sign_of[...].reshape(SEND_MOST * n_dp, 128)
    terms = signs * (products * weights + shift)
    terms = jnp.maximum(terms, 0.0) + jnp.log1p(jnp.exp(-jnp.abs(terms)))
    terms = jnp.where(signs == 0.0, 0.0, terms)
    losses = jnp.sum(terms, axis=0, keepdims=True) / float(n_dp * SEL_DEV)
    losses_out[...] = jnp.where(filled > 0.0, losses, 0.0)

    draining.append(True)
    for act in (place_x, place_y, place_core, wo_x, wo_x_forward, wo_y, wo_core, caps_y, caps_z, caps_core, share):
        act()
    for k in range(SEND_MOST):
        for act in (pix_send, pix_forward, ctx_send, ctx_forward):
            act(k)
    others = arrived.at[pl.ds(0, n_dp - 1)]
    pltpu.make_async_copy(others, others, out_s).wait()


def hand_over(embedded, losses, embedded_out, losses_out):
    embedded_out[...] = embedded[...]
    losses_out[...] = losses[0, :RECV_MOST]


def per_device(
    pixels, selection, destination, patch_weight, position, query_key_value, output_weight, up_weight,
    down_weight, norm_gains, embedding_weight, caption_vectors, loss_params,
):
    n_dp, n_mp = lax.axis_size("dp"), lax.axis_size("mp")
    width, units = up_weight.shape
    share = query_key_value.shape[2]
    patch_rows, values = pixels.shape[1:]
    rows = n_mp * patch_rows
    place_rows = position.shape[0] // (Y * CORES)
    slice_rows = output_weight.shape[0] // (Y * CORES)
    position = position.reshape(CORES, Y, place_rows, width)
    output_weight = output_weight.reshape(CORES, Y, slice_rows, width)
    vmem = pl.BlockSpec(memory_space=pltpu.VMEM)
    far = pl.BlockSpec(memory_space=pl.ANY)
    dma = pltpu.SemaphoreType.DMA
    n = SEND_MOST
    scratch = [
        pltpu.SMEM(selection.shape, jnp.int32), pltpu.SMEM(destination.shape, jnp.int32),
        pltpu.SMEM(loss_params.shape, F32), pltpu.VMEM(norm_gains.shape, F32),
        pltpu.VMEM(pixels.shape, BF16), pltpu.VMEM(patch_weight.shape, BF16),
        pltpu.VMEM(query_key_value.shape, BF16), pltpu.VMEM(up_weight.shape, BF16),
        pltpu.VMEM(down_weight.shape, BF16), pltpu.VMEM(embedding_weight.shape, BF16),
        pltpu.VMEM(caption_vectors.shape, BF16),
        pltpu.VMEM((n, n_mp, patch_rows, values), BF16),
        pltpu.VMEM((n_mp, CORES, Y, place_rows, width), BF16),
        pltpu.VMEM((n_mp, CORES, Y, slice_rows, width), BF16),
        pltpu.VMEM((n, rows, width), F32), pltpu.VMEM((rows, width), BF16),
        pltpu.VMEM((3, rows, share), BF16), pltpu.VMEM((n, n_mp, rows, share), BF16),
        pltpu.VMEM((n + 1, 8, 128), BF16), pltpu.VMEM((CORES, n_dp // (CORES * Y), Y, n + 1, 8, 128), BF16),
        pltpu.VMEM((n * n_dp * 8, 128), BF16), pltpu.VMEM((n, 8, units), F32),
        pltpu.VMEM((n_mp, n, 8, 128), F32),
        pltpu.VMEM((n_dp, 8, 128), BF16), pltpu.VMEM((n_dp, 8, 128), BF16),
        pltpu.VMEM((128, n_dp * 8), BF16), pltpu.VMEM((n, n_dp, 128), F32), pltpu.VMEM((n, n_dp, 128), F32),
        dma((13,)), dma((n, 6)), dma((n, 6)), dma((3,)), dma((3,)), dma((3, 3)), dma((3, 3)), dma((3,)), dma((3,)),
        dma((6,)), dma((6,)), dma((3, 3)), dma((3, 3)), dma((3,)), dma((3,)),
        dma((n, 6)), dma((n, 6)), dma((3,)), dma((3,)), dma((3,)), dma((3,)),
        dma((7,)), dma((7,)), dma, dma, dma, dma, pltpu.SemaphoreType.REGULAR((5,)),
    ]
    embedded, losses = pl.pallas_call(
        functools.partial(body, n_dp, n_mp),
        out_shape=(
            jax.ShapeDtypeStruct((RECV_MOST, width), F32),
            jax.ShapeDtypeStruct((1, 128), F32),
        ),
        in_specs=[far] * 13,
        out_specs=(vmem, vmem),
        scratch_shapes=scratch,
        name="learner",
        compiler_params=pltpu.CompilerParams(
            collective_id=0, has_side_effects=True, vmem_limit_bytes=60 * 1024 * 1024
        ),
    )(
        selection, destination, loss_params, pixels, patch_weight, position, query_key_value, output_weight,
        up_weight, down_weight, norm_gains, embedding_weight, caption_vectors,
    )
    return pl.pallas_call(
        hand_over,
        out_shape=(jax.ShapeDtypeStruct((RECV_MOST, width), F32), jax.ShapeDtypeStruct((RECV_MOST,), F32)),
        name="hand_over",
    )(embedded, losses)


def solution(mesh):
    in_specs = (
        P("dp", "mp", None), P("dp"), P("dp"), P(), P("mp", None), P(None, None, "mp"), P("mp", None),
        P(None, "mp"), P("mp", None), P(), P(), P("dp", None), P(),
    )
    out_specs = (P("dp", None), P("dp"))
    return jax.shard_map(per_device, mesh=mesh, in_specs=in_specs, out_specs=out_specs, check_vma=False)
```
